32 devices in a mesh: shot: 4 (over y, core), tile: 8 (over z, x).
Axes of the slice: x: 2, y: 2, z: 4, core: 2. Of those that a mesh axis runs over, the one named last changes fastest.
Arguments:
- source: bfloat16 [64, 1, 32, 32, 128], P(('shot', 'tile')), may hold values from -6 to 6
- receiver: bfloat16 [64, 1, 32, 32, 128], P(('shot', 'tile')), may hold values from -6 to 6
- corners: int32 [64, 2], P(('shot', 'tile')), may hold values from 0 to 224, as said below
Outputs:
- filtered: float32 [32, 256, 256], P('tile', 'shot')
The draws below stay inside these ranges and needn't reach their ends.
Inputs may be any that keep to these rules, and one draw needn't show every extreme that they name: corners[s, 0] is at most 224 and corners[s, 1] at most 128, so every box lies inside the image.
All inputs are finite; a program needn't handle non-finite values.
Results may differ from the reference program's by a relative error of at most 0.0003.
Values may be sent and summed in bfloat16 or wider, within the bound.
A program may use at most 64 MiB of HBM per device.

```python
import jax
import jax.numpy as jnp
from jax import lax

NT = 1
X = 256
Y = 256
BX = 32
BY = 128
SHOTS = 64
Z = 32


def draw_corners(key, part):
    first_key, second_key = jax.random.split(jax.random.fold_in(key, 17))
    row_start = jax.random.randint(first_key, (SHOTS, 1), 0, X - BX + 1)
    col_start = jax.random.randint(second_key, (SHOTS, 1), 0, Y - BY + 1)
    return jnp.concatenate((row_start, col_start), axis=1).astype(jnp.int32)


def level_of(stream_key, dims, cuts, least, largest):
    factor_of = 1.0
    for axis_at, shards_of in cuts:
        steps = jax.random.uniform(jax.random.fold_in(jax.random.fold_in(stream_key, 6), axis_at), (shards_of,), jnp.float32, least / len(cuts), largest / len(cuts))
        factor_of = factor_of * jnp.repeat(jnp.exp(steps), dims[axis_at] // shards_of).reshape((-1,) + (1,) * (len(dims) - 1 - axis_at))
    return factor_of


def bell_draw(key, dims, spread, reach, cuts=(), kind=jnp.bfloat16):
    result = jax.random.normal(key, dims, jnp.float32) * spread
    if len(cuts) > 0:
        result = level_of(key, dims, cuts, -0.22, 0.18) * result
    return jnp.clip(result, min=-reach, max=reach).astype(kind)


def setup_inputs(seed: int = 0) -> dict:
    keys = jax.random.split(jax.random.key(seed), 4)
    return {
        "source": bell_draw(keys[0], (SHOTS, NT, Z, BX, BY), 1.0, 6.0, ((0, 32),)),
        "receiver": bell_draw(keys[1], (SHOTS, NT, Z, BX, BY), 1.0, 6.0, ((0, 32),)),
        "corners": draw_corners(jax.random.fold_in(keys[3], 71), 0),
    }


damping = 1.0


def reference(source, receiver, corners):
    def place(shot, totals):
        image, lights = totals
        wave = lax.dynamic_index_in_dim(source, shot, 0, keepdims=False).astype(jnp.float32)
        back = lax.dynamic_index_in_dim(receiver, shot, 0, keepdims=False).astype(jnp.float32)
        partial_value = jnp.sum(wave * back, axis=0)
        light = jnp.sum(wave * wave, axis=0)
        start = (jnp.int32(0), corners[shot, 0].astype(jnp.int32), corners[shot, 1].astype(jnp.int32))
        image = lax.dynamic_update_slice(image, lax.dynamic_slice(image, start, (Z, BX, BY)) + partial_value, start)
        lights = lax.dynamic_update_slice(lights, lax.dynamic_slice(lights, start, (Z, BX, BY)) + light, start)
        return image, lights

    empty = jnp.zeros((Z, X, Y), jnp.float32)
    image, lights = lax.fori_loop(0, SHOTS, place, (empty, empty))
    normal = image / (damping + lights)
    padded = jnp.pad(normal, 1)
    beside = padded[2:, 1:-1, 1:-1] + padded[:-2, 1:-1, 1:-1]
    beside = beside + padded[1:-1, 2:, 1:-1] + padded[1:-1, :-2, 1:-1]
    beside = beside + padded[1:-1, 1:-1, 2:] + padded[1:-1, 1:-1, :-2]
    return beside - 6.0 * normal
```

```python
import functools

import jax
import jax.numpy as jnp
from jax import lax
from jax.experimental import pallas as pl
from jax.experimental.pallas import tpu as pltpu
from jax.sharding import PartitionSpec as P

X = 256
Y = 256
LANES = 128

damping = 1.0


def partner(index, k, count):
    if count & (count - 1):
        return lax.rem(index + k, count)
    bit = 1
    result = index
    while bit < count:
        if k & bit:
            result = result + bit * (1 - 2 * lax.rem(index // bit, 2))
        bit *= 2
    return result


def plan(depth):
    if depth < 3:
        return list(range(depth)), []
    return [0, depth - 1], list(range(1, depth - 1))


def kernel(
    ns, nt, src, rcv, cor, out, sbuf, rx, cbuf, csm, boxes, acc, r1, r2, mbuf, mx, nrm, hx, hz, rows,
    in_sem, rx_send, rx_recv, c_send, c_recv, c_local,
    s1_send, s1_recv, s2_send, s2_recv, m_send, m_recv, row_send, row_recv, face_send, face_recv,
):
    depth, strip, width = nrm.shape
    spd, samples = src.shape[0], src.shape[1]
    box_rows = src.shape[3]
    halves = width // LANES
    whole, split = plan(depth)
    shots = nt * spd
    block = min(box_rows, strip)
    per_strip = strip // block
    half_ns = ns // 2
    half_nt = nt // 2
    shot = lax.axis_index("shot")
    tile = lax.axis_index("tile")
    core = lax.rem(shot, 2)
    pair = shot // 2
    other = 1 - core
    place_in_half = lax.rem(tile, half_nt)
    base = tile - place_in_half
    mirror = lax.rem(tile + half_nt, nt)

    nw, nb = len(whole), len(split)
    full = {p: n for n, p in enumerate(whole)}
    own = {p: nw + n for n, p in enumerate(split)}
    far = {p: nw + nb + n for n, p in enumerate(split)}
    units = {u: (p, nt) for p, u in full.items()}
    units.update({u: (p, half_nt) for p, u in own.items()})
    units.update({u: (p, half_nt) for p, u in far.items()})

    barrier = pltpu.get_barrier_semaphore()
    for k in range(1, ns):
        pl.semaphore_signal(barrier, inc=1, device_id={"shot": lax.rem(shot + k, ns)})
    for k in range(1, nt):
        pl.semaphore_signal(barrier, inc=1, device_id={"tile": lax.rem(tile + k, nt)})

    for w, ref in enumerate((src, rcv)):
        for i in range(spd):
            for n in range(samples):
                pltpu.make_async_copy(ref.at[i, n], sbuf.at[:, w, i, n], in_sem).start()
    pltpu.make_async_copy(cor, cbuf.at[tile], c_recv).start()
    for u, (p, count) in units.items():
        slab = mirror if u in far.values() else tile
        slot = tile if count == nt else place_in_half
        for w, ref in enumerate((src, rcv)):
            pltpu.make_async_copy(ref.at[:, :, slab * depth + p], rx.at[u, slot, w], rx_recv.at[u]).start()
    pltpu.make_async_copy(sbuf, sbuf, in_sem).wait()

    pl.semaphore_wait(barrier, ns - 1 + nt - 1)

    for k in range(nt - 1, 0, -1):
        pltpu.make_async_remote_copy(
            src_ref=cor, dst_ref=cbuf.at[tile], send_sem=c_send, recv_sem=c_recv,
            device_id={"tile": partner(tile, k, nt)},
        ).start()

    def send_near(u):
        p = units[u][0]
        for k in range(half_nt - 1, 0, -1):
            to = base + partner(place_in_half, k, half_nt)
            slab = lax.rem(to + half_nt, nt) if u in far.values() else to
            slot = tile if units[u][1] == nt else place_in_half
            pltpu.make_async_remote_copy(
                src_ref=sbuf.at[slab * depth + p], dst_ref=rx.at[u, slot],
                send_sem=rx_send.at[u], recv_sem=rx_recv.at[u], device_id={"tile": to},
            ).start()

    def send_far(u):
        p = units[u][0]
        for k in range(half_nt):
            to = (half_nt - base) + partner(place_in_half, k, half_nt)
            pltpu.make_async_remote_copy(
                src_ref=sbuf.at[to * depth + p], dst_ref=rx.at[u, tile],
                send_sem=rx_send.at[u], recv_sem=rx_recv.at[u], device_id={"tile": to},
            ).start()

    for p in split:
        send_near(far[p])
    for p in whole:
        send_far(full[p])
    for p in whole:
        send_near(full[p])
    for p in split:
        send_near(own[p])

    edges = (
        (shot < ns - 1, shot > 0, {"shot": lax.rem(shot + 1, ns)}),
        (shot > 0, shot < ns - 1, {"shot": lax.rem(shot + ns - 1, ns)}),
    )
    faces = (
        (tile < nt - 1, tile > 0, {"tile": lax.rem(tile + 1, nt)}, depth - 1),
        (tile > 0, tile < nt - 1, {"tile": lax.rem(tile + nt - 1, nt)}, 0),
    )
    for d in range(2):
        @pl.when(jnp.logical_not(edges[d][1]))
        def _(d=d):
            hx[d] = jnp.zeros((depth, 1, width), jnp.float32)

        @pl.when(jnp.logical_not(faces[d][1]))
        def _(d=d):
            hz[d] = jnp.zeros((strip, width), jnp.float32)

    def edge_copy(d, p):
        return pltpu.make_async_remote_copy(
            src_ref=rows.at[d, p], dst_ref=hx.at[d, p],
            send_sem=row_send.at[d, p], recv_sem=row_recv.at[d, p], device_id=edges[d][2],
        )

    def face_copy(d):
        return pltpu.make_async_remote_copy(
            src_ref=nrm.at[faces[d][3]], dst_ref=hz.at[d],
            send_sem=face_send.at[d], recv_sem=face_recv.at[d], device_id=faces[d][2],
        )

    def cross_copy(p):
        n = split.index(p)
        return pltpu.make_async_remote_copy(
            src_ref=mbuf.at[n], dst_ref=mx.at[n],
            send_sem=m_send.at[n], recv_sem=m_recv.at[n], device_id={"tile": mirror},
        )

    zero = jnp.zeros((block, LANES), jnp.float32)

    def clear(s, carry):
        for q in range(2):
            for h in range(halves):
                boxes[s, q, h, pl.ds(0, block), :] = zero
                boxes[s, q, h, pl.ds(block + box_rows, block), :] = zero
        return carry

    lax.fori_loop(0, shots, clear, 0)

    pltpu.make_async_copy(cbuf, cbuf, c_recv).wait()
    to_scalar = pltpu.make_async_copy(cbuf, csm, c_local)
    to_scalar.start()
    to_scalar.wait()

    lane = lax.broadcasted_iota(jnp.int32, (box_rows, LANES), 1)

    def expand(u):
        first_tile = 0 if units[u][1] == nt else base

        def peer(t, carry):
            for i in range(spd):
                s = t * spd + i
                col = csm[first_tile + t, i, 1]
                turn = lax.rem(col, LANES)
                image = jnp.zeros((box_rows, LANES), jnp.float32)
                light = image
                for n in range(samples):
                    wave = rx[u, t, 0, i, n].astype(jnp.float32)
                    back = rx[u, t, 1, i, n].astype(jnp.float32)
                    image = wave * back if n == 0 else image + wave * back
                    light = wave * wave if n == 0 else light + wave * wave
                image = pltpu.roll(image, turn, 1)
                light = pltpu.roll(light, turn, 1)
                for h in range(halves):
                    at = lane + (h * LANES - col)
                    inside = (at >= 0) & (at < LANES)
                    boxes[s, 0, h, pl.ds(block, box_rows), :] = jnp.where(inside, image, 0.0)
                    boxes[s, 1, h, pl.ds(block, box_rows), :] = jnp.where(inside, light, 0.0)
            return carry

        lax.fori_loop(0, units[u][1], peer, 0)

    def place(u, parity):
        first_tile = 0 if units[u][1] == nt else base

        def one(n, carry):
            j = 2 * (n // per_strip) + parity
            at = lax.rem(n, per_strip) * block
            first = j * strip + at + block
            total = [[None] * halves for _ in range(2)]
            for s in range(units[u][1] * spd):
                start = jnp.clip(first - csm[first_tile + s // spd, s % spd, 0], 0, box_rows + block)
                for q in range(2):
                    for h in range(halves):
                        piece = boxes[s, q, h, pl.ds(start, block), :]
                        total[q][h] = piece if s == 0 else total[q][h] + piece
            for q in range(2):
                for h in range(halves):
                    acc[u, j, q, pl.ds(at, block), pl.ds(h * LANES, LANES)] = total[q][h]
            return carry

        lax.fori_loop(0, half_ns * per_strip, one, 0)

    def stage1(u):
        for i in range(half_ns):
            pltpu.make_async_remote_copy(
                src_ref=acc.at[u, 2 * i + other],
                dst_ref=r1.at[u, i],
                send_sem=s1_send.at[u],
                recv_sem=s1_recv.at[u],
                device_id={"shot": 2 * pair + other},
            ).start()

    def gather(u):
        got = rx.at[u] if units[u][1] == nt else rx.at[u, pl.ds(0, half_nt)]
        pltpu.make_async_copy(got, got, rx_recv.at[u]).wait()
        expand(u)
        place(u, other)
        stage1(u)
        place(u, core)

    def stage2(u):
        pltpu.make_async_copy(r1.at[u], r1.at[u], s1_recv.at[u]).wait()
        for k in range(1, half_ns):
            to = lax.rem(pair + k, half_ns)
            j = 2 * to + core
            acc[u, j] = acc[u, j] + r1[u, to]
            pltpu.make_async_remote_copy(
                src_ref=acc.at[u, j],
                dst_ref=r2.at[u, k - 1],
                send_sem=s2_send.at[u],
                recv_sem=s2_recv.at[u],
                device_id={"shot": j},
            ).start()

    def totals(u):
        pltpu.make_async_copy(r2.at[u], r2.at[u], s2_recv.at[u]).wait()
        image = acc[u, shot, 0] + r1[u, pair, 0]
        light = acc[u, shot, 1] + r1[u, pair, 1]
        for k in range(half_ns - 1):
            image = image + r2[u, k, 0]
            light = light + r2[u, k, 1]
        return image, light

    def cross(p):
        n = split.index(p)
        image, light = totals(far[p])
        mbuf[n, 0] = image
        mbuf[n, 1] = light
        cross_copy(p).start()

    def finish(p):
        if p in full:
            image, light = totals(full[p])
        else:
            n = split.index(p)
            image, light = totals(own[p])
            cross_copy(p).wait_recv()
            image = image + mx[n, 0]
            light = light + mx[n, 1]
        normal = image / (damping + light)
        nrm[p] = normal
        rows[0, p] = normal[strip - 1 :, :]
        rows[1, p] = normal[:1, :]
        for d in range(2):
            @pl.when(edges[d][0])
            def _(d=d):
                edge_copy(d, p).start()

            if p == faces[d][3]:
                @pl.when(faces[d][0])
                def _(d=d):
                    face_copy(d).start()

    row = lax.broadcasted_iota(jnp.int32, (strip, width), 0)
    column = lax.broadcasted_iota(jnp.int32, (strip, width), 1)

    def lateral(p):
        center = nrm[p]
        before = jnp.where(row == 0, 0.0, pltpu.roll(center, 1, 0))
        after = jnp.where(row == strip - 1, 0.0, pltpu.roll(center, strip - 1, 0))
        left = jnp.where(column == 0, 0.0, pltpu.roll(center, 1, 1))
        right = jnp.where(column == width - 1, 0.0, pltpu.roll(center, width - 1, 1))
        return before + after + left + right - 6.0 * center

    def wait_edges(p):
        for d in range(2):
            @pl.when(edges[d][1])
            def _(d=d):
                edge_copy(d, p).wait_recv()

    def add_edges(p):
        out[p, pl.ds(0, 1), :] = out[p, pl.ds(0, 1), :] + hx[0, p]
        out[p, pl.ds(strip - 1, 1), :] = out[p, pl.ds(strip - 1, 1), :] + hx[1, p]

    def near_planes(p):
        return [q for q in (p - 1, p + 1) if 0 <= q < depth]

    def base_plane(p, known):
        value = lateral(p)
        for q in near_planes(p):
            if q in known:
                value = value + nrm[q]
        for d in range(2):
            if p == (depth - 1 if d else 0):
                @pl.when(faces[d][1])
                def _(d=d):
                    face_copy(d).wait_recv()
                value = value + hz[d]
        out[p] = value
        wait_edges(p)
        add_edges(p)

    first, last = split[0], split[-1]
    middle = split[:-1]

    for p in split:
        gather(far[p])
    for p in split:
        stage2(far[p])
    rest = [full[whole[0]]] + [own[p] for p in middle] + [full[p] for p in whole[1:]] + [own[last]]
    for n, u in enumerate(rest):
        gather(u)
        if n < nb:
            cross(split[n])
        if n >= 1 and units[rest[n - 1]][1] == nt:
            pass
        stage2(u)
    for p in whole:
        finish(p)
    for p in middle:
        finish(p)
    known = whole + middle
    for p in known:
        base_plane(p, known)
    finish(last)
    for p in near_planes(last):
        out[p] = out[p] + nrm[last]
    base_plane(last, known)

    for d in range(2):
        @pl.when(edges[d][0])
        def _(d=d):
            for p in range(depth):
                edge_copy(d, p).wait_send()

        @pl.when(faces[d][0])
        def _(d=d):
            face_copy(d).wait_send()

    sent = cbuf.at[pl.ds(0, nt - 1)]
    pltpu.make_async_copy(sent, sent, c_send).wait()
    for u, (p, count) in units.items():
        sent = rx.at[u, pl.ds(0, count - 1)]
        pltpu.make_async_copy(sent, sent, rx_send.at[u]).wait()
        pltpu.make_async_copy(r1.at[u], r1.at[u], s1_send.at[u]).wait()
        pltpu.make_async_copy(r2.at[u], r2.at[u], s2_send.at[u]).wait()
    for p in split:
        cross_copy(p).wait_send()


def solution(mesh):
    ns, nt = mesh.shape["shot"], mesh.shape["tile"]

    def step(source, receiver, corners):
        spd, samples, full_depth, box_rows, box_cols = source.shape
        depth = full_depth // nt
        strip = X // ns
        block = min(box_rows, strip)
        half_ns = ns // 2
        whole, split = plan(depth)
        nb = len(split)
        count = len(whole) + 2 * nb
        vmem = pltpu.VMEM
        dma = pltpu.SemaphoreType.DMA
        f32 = jnp.float32
        return pl.pallas_call(
            functools.partial(kernel, ns, nt),
            out_shape=jax.ShapeDtypeStruct((depth, strip, Y), f32),
            in_specs=[pl.BlockSpec(memory_space=pl.ANY)] * 3,
            out_specs=pl.BlockSpec(memory_space=pltpu.VMEM),
            scratch_shapes=[
                vmem((full_depth, 2, spd, samples, box_rows, box_cols), jnp.bfloat16),
                vmem((count, nt, 2, spd, samples, box_rows, box_cols), jnp.bfloat16),
                vmem((nt, spd, 2), jnp.int32),
                pltpu.SMEM((nt, spd, 2), jnp.int32),
                vmem((nt * spd, 2, Y // LANES, box_rows + 2 * block, LANES), f32),
                vmem((count, ns, 2, strip, Y), f32),
                vmem((count, half_ns, 2, strip, Y), f32),
                vmem((count, half_ns - 1, 2, strip, Y), f32),
                vmem((max(nb, 1), 2, strip, Y), f32),
                vmem((max(nb, 1), 2, strip, Y), f32),
                vmem((depth, strip, Y), f32),
                vmem((2, depth, 1, Y), f32),
                vmem((2, strip, Y), f32),
                vmem((2, depth, 1, Y), f32),
                dma,
                dma((count,)),
                dma((count,)),
                dma,
                dma,
                dma,
                dma((count,)),
                dma((count,)),
                dma((count,)),
                dma((count,)),
                dma((max(nb, 1),)),
                dma((max(nb, 1),)),
                dma((2, depth)),
                dma((2, depth)),
                dma((2,)),
                dma((2,)),
            ],
            compiler_params=pltpu.CompilerParams(
                collective_id=0, has_side_effects=True, vmem_limit_bytes=54700 * 1024
            ),
        )(source, receiver, corners)

    return jax.shard_map(
        step,
        mesh=mesh,
        in_specs=(
            P(("shot", "tile"), None, None, None, None),
            P(("shot", "tile"), None, None, None, None),
            P(("shot", "tile"), None),
        ),
        out_specs=P("tile", "shot", None),
        check_vma=False,
    )
```

```python
import functools

import jax
import jax.numpy as jnp
from jax import lax
from jax.experimental import pallas as pl
from jax.experimental.pallas import tpu as pltpu
from jax.sharding import PartitionSpec as P

X = 256
Y = 256
LANES = 128

damping = 1.0


def partner(index, k, count):
    if count & (count - 1):
        return lax.rem(index + k, count)
    bit = 1
    result = index
    while bit < count:
        if k & bit:
            result = result + bit * (1 - 2 * lax.rem(index // bit, 2))
        bit *= 2
    return result


def partner_back(index, k, count):
    if count & (count - 1):
        return lax.rem(index + count - k, count)
    return partner(index, k, count)


def plan(depth):
    if depth < 3:
        return list(range(depth)), []
    return [0, depth - 1], list(range(1, depth - 1))


def kernel(
    ns, nt, src, rcv, cor, out, sbuf, rxw, rxh, cbuf, csm, cby, csy, boxes,
    acc, r1, r2, hacc, hr1, hal, hal1, mbuf, mx, mhal, mhx, nrm, hx, hz, rows,
    in_sem, rxw_send, rxw_recv, rxh_send, rxh_recv, ry_send, ry_recv,
    c_send, c_recv, cn_send, cn_recv, cy_send, cy_recv, c_local,
    s1_send, s1_recv, s2_send, s2_recv, h1_send, h1_recv, m_send, m_recv,
    row_send, row_recv, face_send, face_recv, known_sem,
):
    depth, strip, width = nrm.shape
    spd, samples = src.shape[0], src.shape[1]
    box_rows = src.shape[3]
    halves = width // LANES
    whole, split = plan(depth)
    block = min(box_rows, strip)
    per_strip = strip // block
    half_ns = ns // 2
    half_nt = nt // 2
    shot = lax.axis_index("shot")
    tile = lax.axis_index("tile")
    core = lax.rem(shot, 2)
    pair = shot // 2
    other = 1 - core
    mine = lax.rem(tile, half_nt)
    base = tile - mine
    mirror = lax.rem(tile + half_nt, nt)
    twin = {"shot": 2 * pair + other}
    nb = len(split)
    far = range(nb)
    own = range(nb, 2 * nb)
    plane = split + split

    def peer_shot(m):
        return {"shot": 2 * lax.rem(pair + m, half_ns) + core}

    def slab_of(u, to):
        return lax.rem(to + half_nt, nt) if u in far else to

    barrier = pltpu.get_barrier_semaphore()
    for k in range(1, ns):
        pl.semaphore_signal(barrier, inc=1, device_id={"shot": lax.rem(shot + k, ns)})
    column, side = tile // 2, lax.rem(tile, 2)
    columns = nt // 2
    around = (
        (None, {"tile": tile + 1 - 2 * side}),
        (column > 0, {"tile": lax.rem(tile + nt - 2, nt)}),
        (column < columns - 1, {"tile": lax.rem(tile + 2, nt)}),
    )

    def greet(sem):
        for there, who in around:
            if there is None:
                pl.semaphore_signal(sem, inc=1, device_id=who)
            else:
                @pl.when(there)
                def _(who=who):
                    pl.semaphore_signal(sem, inc=1, device_id=who)

    def await_greetings(sem, more):
        pl.semaphore_wait(sem, more + 1 + jnp.minimum(column, 1) + jnp.minimum(columns - 1 - column, 1))

    def learn(r):
        await_greetings(known_sem.at[r], 0)
        if r + 1 < known_sem.shape[0]:
            greet(known_sem.at[r + 1])

    greet(barrier)

    for w, ref in enumerate((src, rcv)):
        for i in range(spd):
            for n in range(samples):
                pltpu.make_async_copy(ref.at[i, n], sbuf.at[:, w, i, n], in_sem).start()
    pltpu.make_async_copy(cor, cbuf.at[tile], c_recv).start()
    pltpu.make_async_copy(cor, cby.at[0, mine], cn_recv).start()
    for w, ref in enumerate((src, rcv)):
        for u, p in enumerate(plane):
            pltpu.make_async_copy(
                ref.at[:, :, slab_of(u, tile) * depth + p], rxh.at[u, 0, mine, w], rxh_recv.at[u, 0]
            ).start()
        for u, p in enumerate(whole):
            pltpu.make_async_copy(ref.at[:, :, tile * depth + p], rxw.at[u, tile, w], rxw_recv.at[u]).start()
    pltpu.make_async_copy(sbuf, sbuf, in_sem).wait()

    await_greetings(barrier, ns - 1)
    greet(known_sem.at[0])

    def remote(src_ref, dst_ref, send_sem, recv_sem, device_id):
        pltpu.make_async_remote_copy(
            src_ref=src_ref, dst_ref=dst_ref, send_sem=send_sem, recv_sem=recv_sem, device_id=device_id
        ).start()

    def steps(to):
        return abs(to // 2 - column) + abs(lax.rem(to, 2) - side)

    def near_half(u, when=None):
        for k in range(1, half_nt):
            to = base + partner(mine, k, half_nt)
            guarded(when, to, lambda k=k, to=to: remote(
                sbuf.at[slab_of(u, to) * depth + plane[u]], rxh.at[u, 0, mine],
                rxh_send.at[u], rxh_recv.at[u, k], {"tile": to},
            ))

    def guarded(when, to, send):
        if when is None:
            send()
        else:
            @pl.when(when(steps(to)))
            def _():
                send()

    def own_half(u):
        for m in range(1, half_ns):
            remote(
                sbuf.at[slab_of(u, tile) * depth + plane[u]], rxh.at[u, m, mine],
                ry_send.at[u], ry_recv.at[u], peer_shot(m),
            )

    def relay(u):
        for k in range(1, half_nt):
            slot = partner_back(mine, k, half_nt)
            got = rxh.at[u, 0, slot]
            pltpu.make_async_copy(got, got, rxh_recv.at[u, k]).wait()
            for m in range(1, half_ns):
                remote(got, rxh.at[u, m, slot], ry_send.at[u], ry_recv.at[u], peer_shot(m))

    def near_whole(u, when=None):
        for k in range(1, half_nt):
            to = base + partner(mine, k, half_nt)
            guarded(when, to, lambda to=to: remote(
                sbuf.at[to * depth + whole[u]], rxw.at[u, tile], rxw_send.at[u], rxw_recv.at[u], {"tile": to}
            ))

    def far_whole(u, when=None):
        for k in range(half_nt):
            to = (half_nt - base) + partner(mine, k, half_nt)
            guarded(when, to, lambda to=to: remote(
                sbuf.at[to * depth + whole[u]], rxw.at[u, tile], rxw_send.at[u], rxw_recv.at[u], {"tile": to}
            ))

    def corners(when):
        for k in range(1, half_nt):
            to = base + partner(mine, k, half_nt)
            guarded(when, to, lambda to=to: remote(cor, cby.at[0, mine], cn_send, cn_recv, {"tile": to}))
        for k in range(1, nt):
            to = partner(tile, k, nt)
            guarded(when, to, lambda to=to: remote(cor, cbuf.at[tile], c_send, c_recv, {"tile": to}))

    for level in (1, 2, 3):
        if level == 1:
            when = lambda d: d == 1
        elif level == 2:
            learn(0)
            when = lambda d: d == 2
        else:
            for r in range(1, known_sem.shape[0]):
                learn(r)
            when = lambda d: d > 2
        corners(when)
        near_half(far[0], when)
        far_whole(0, when)
        if level == 1:
            for u in range(2 * nb):
                own_half(u)
    for u in far[1:]:
        near_half(u)
    near_whole(0)
    near_half(own[0])
    far_whole(1)
    near_whole(1)
    for u in own[1:]:
        near_half(u)

    edges = (
        (shot < ns - 1, shot > 0, {"shot": lax.rem(shot + 1, ns)}),
        (shot > 0, shot < ns - 1, {"shot": lax.rem(shot + ns - 1, ns)}),
    )
    faces = (
        (tile < nt - 1, tile > 0, {"tile": lax.rem(tile + 1, nt)}, depth - 1),
        (tile > 0, tile < nt - 1, {"tile": lax.rem(tile + nt - 1, nt)}, 0),
    )
    for d in range(2):
        @pl.when(jnp.logical_not(edges[d][1]))
        def _(d=d):
            hx[d] = jnp.zeros((depth, 1, width), jnp.float32)

        @pl.when(jnp.logical_not(faces[d][1]))
        def _(d=d):
            hz[d] = jnp.zeros((strip, width), jnp.float32)

    def edge_copy(d, p):
        return pltpu.make_async_remote_copy(
            src_ref=rows.at[d, p], dst_ref=hx.at[d, p],
            send_sem=row_send.at[d, p], recv_sem=row_recv.at[d, p], device_id=edges[d][2],
        )

    def face_copy(d):
        return pltpu.make_async_remote_copy(
            src_ref=nrm.at[faces[d][3]], dst_ref=hz.at[d],
            send_sem=face_send.at[d], recv_sem=face_recv.at[d], device_id=faces[d][2],
        )

    def cross_copies(n):
        pieces = []
        for g, (a, b) in enumerate(((mbuf, mx), (mhal, mhx))):
            pieces.append(pltpu.make_async_remote_copy(
                src_ref=a.at[n], dst_ref=b.at[n],
                send_sem=m_send.at[n, g], recv_sem=m_recv.at[n, g], device_id={"tile": mirror},
            ))
        return pieces

    zero = jnp.zeros((block, LANES), jnp.float32)

    def clear(s, carry):
        for q in range(2):
            for h in range(halves):
                boxes[s, q, h, pl.ds(0, block), :] = zero
                boxes[s, q, h, pl.ds(block + box_rows, block), :] = zero
        return carry

    lax.fori_loop(0, boxes.shape[0], clear, 0)

    lane = lax.broadcasted_iota(jnp.int32, (box_rows, LANES), 1)

    def expand_one(s, col, wave_of, back_of):
        turn = lax.rem(col, LANES)
        image = jnp.zeros((box_rows, LANES), jnp.float32)
        light = image
        for n in range(samples):
            wave = wave_of(n).astype(jnp.float32)
            back = back_of(n).astype(jnp.float32)
            image = wave * back if n == 0 else image + wave * back
            light = wave * wave if n == 0 else light + wave * wave
        image = pltpu.roll(image, turn, 1)
        light = pltpu.roll(light, turn, 1)
        for h in range(halves):
            at = lane + (h * LANES - col)
            inside = (at >= 0) & (at < LANES)
            boxes[s, 0, h, pl.ds(block, box_rows), :] = jnp.where(inside, image, 0.0)
            boxes[s, 1, h, pl.ds(block, box_rows), :] = jnp.where(inside, light, 0.0)

    def expand_whole(u):
        def peer(t, carry):
            for i in range(spd):
                expand_one(
                    t * spd + i, csm[t, i, 1],
                    lambda n: rxw[u, t, 0, i, n], lambda n: rxw[u, t, 1, i, n],
                )
            return carry

        lax.fori_loop(0, nt, peer, 0)

    def expand_half(u):
        for m in range(half_ns):
            def peer(t, carry):
                for i in range(spd):
                    expand_one(
                        (m * half_nt + t) * spd + i, csy[m, t, i, 1],
                        lambda n: rxh[u, m, t, 0, i, n], lambda n: rxh[u, m, t, 1, i, n],
                    )
                return carry

            lax.fori_loop(0, half_nt, peer, 0)

    whole_rows = [(s, lambda s=s: csm[s // spd, s % spd, 0]) for s in range(nt * spd)]
    half_rows = [
        ((m * half_nt + t) * spd + i, lambda m=m, t=t, i=i: csy[m, t, i, 0])
        for m in range(half_ns) for t in range(half_nt) for i in range(spd)
    ]

    def stack(corner_rows, first, count):
        total = [[None] * halves for _ in range(2)]
        for s, corner in corner_rows:
            start = jnp.clip(first + block - corner(), 0, box_rows + block)
            for q in range(2):
                for h in range(halves):
                    piece = boxes[s, q, h, pl.ds(start, count), :]
                    total[q][h] = piece if total[q][h] is None else total[q][h] + piece
        return total

    def place_whole(u, parity):
        def one(n, carry):
            j = 2 * (n // per_strip) + parity
            at = lax.rem(n, per_strip) * block
            total = stack(whole_rows, j * strip + at, block)
            for q in range(2):
                for h in range(halves):
                    acc[u, j, q, pl.ds(at, block), pl.ds(h * LANES, LANES)] = total[q][h]
            return carry

        lax.fori_loop(0, half_ns * per_strip, one, 0)

    def place_half(u, parity):
        top = (2 * pair + parity) * strip

        def one(n, carry):
            at = n * block
            total = stack(half_rows, top + at, block)
            for q in range(2):
                for h in range(halves):
                    hacc[u, parity, q, pl.ds(at, block), pl.ds(h * LANES, LANES)] = total[q][h]
            return carry

        lax.fori_loop(0, per_strip, one, 0)
        for d, first in enumerate((top - 1, top + strip)):
            total = stack(half_rows, first, 1)
            for q in range(2):
                for h in range(halves):
                    hal[u, parity, pl.ds(2 * q + d, 1), pl.ds(h * LANES, LANES)] = total[q][h]

    def gather_whole(u):
        pltpu.make_async_copy(rxw.at[u], rxw.at[u], rxw_recv.at[u]).wait()
        expand_whole(u)
        place_whole(u, other)
        for i in range(half_ns):
            remote(acc.at[u, 2 * i + other], r1.at[u, i], s1_send.at[u], s1_recv.at[u], twin)
        place_whole(u, core)

    def gather_half(u):
        got = rxh.at[u, 0, mine]
        pltpu.make_async_copy(got, got, rxh_recv.at[u, 0]).wait()
        got = rxh.at[u, pl.ds(1, half_ns - 1)]
        pltpu.make_async_copy(got, got, ry_recv.at[u]).wait()
        expand_half(u)
        place_half(u, other)
        remote(hacc.at[u, other], hr1.at[u], h1_send.at[u, 0], h1_recv.at[u, 0], twin)
        remote(hal.at[u, other], hal1.at[u], h1_send.at[u, 1], h1_recv.at[u, 1], twin)
        place_half(u, core)

    def wait_twin(u):
        pltpu.make_async_copy(hr1.at[u], hr1.at[u], h1_recv.at[u, 0]).wait()
        pltpu.make_async_copy(hal1.at[u], hal1.at[u], h1_recv.at[u, 1]).wait()

    def stage2(u):
        pltpu.make_async_copy(r1.at[u], r1.at[u], s1_recv.at[u]).wait()
        for k in range(1, half_ns):
            to = lax.rem(pair + k, half_ns)
            j = 2 * to + core
            acc[u, j] = acc[u, j] + r1[u, to]
            remote(acc.at[u, j], r2.at[u, k - 1], s2_send.at[u], s2_recv.at[u], {"shot": j})

    def cross(n):
        u = far[n]
        wait_twin(u)
        mhal[n] = hal[u, core] + hal1[u]
        mbuf[n] = hacc[u, core] + hr1[u]
        for copy in reversed(cross_copies(n)):
            copy.start()

    def finish_whole(u):
        p = whole[u]
        pltpu.make_async_copy(r2.at[u], r2.at[u], s2_recv.at[u]).wait()
        image = acc[u, shot, 0] + r1[u, pair, 0]
        light = acc[u, shot, 1] + r1[u, pair, 1]
        for k in range(half_ns - 1):
            image = image + r2[u, k, 0]
            light = light + r2[u, k, 1]
        normal = image / (damping + light)
        nrm[p] = normal
        rows[0, p] = normal[strip - 1 :, :]
        rows[1, p] = normal[:1, :]
        for d in range(2):
            @pl.when(edges[d][0])
            def _(d=d):
                edge_copy(d, p).start()

            if p == faces[d][3]:
                @pl.when(faces[d][0])
                def _(d=d):
                    face_copy(d).start()

    def finish_half(n):
        p, u = split[n], own[n]
        wait_twin(u)
        for copy in cross_copies(n):
            copy.wait_recv()
        image = (hacc[u, core, 0] + hr1[u, 0]) + mx[n, 0]
        light = (hacc[u, core, 1] + hr1[u, 1]) + mx[n, 1]
        nrm[p] = image / (damping + light)
        rim = hal[u, core] + hal1[u] + mhx[n]
        rim = rim[0:2, :] / (damping + rim[2:4, :])
        hx[0, p] = rim[0:1, :]
        hx[1, p] = rim[1:2, :]

    row = lax.broadcasted_iota(jnp.int32, (strip, width), 0)
    lanes = lax.broadcasted_iota(jnp.int32, (strip, width), 1)

    def lateral(p):
        center = nrm[p]
        before = jnp.where(row == 0, hx[0, p], pltpu.roll(center, 1, 0))
        after = jnp.where(row == strip - 1, hx[1, p], pltpu.roll(center, strip - 1, 0))
        left = jnp.where(lanes == 0, 0.0, pltpu.roll(center, 1, 1))
        right = jnp.where(lanes == width - 1, 0.0, pltpu.roll(center, width - 1, 1))
        return before + after + left + right - 6.0 * center

    def near_planes(p):
        return [q for q in (p - 1, p + 1) if 0 <= q < depth]

    def base_plane(p, known):
        if p in whole:
            for d in range(2):
                @pl.when(edges[d][1])
                def _(d=d):
                    edge_copy(d, p).wait_recv()
        value = lateral(p)
        for q in near_planes(p):
            if q in known:
                value = value + nrm[q]
        for d in range(2):
            if p == (depth - 1 if d else 0):
                @pl.when(faces[d][1])
                def _(d=d):
                    face_copy(d).wait_recv()
                value = value + hz[d]
        out[p] = value

    last = split[-1]
    middle = split[:-1]

    pltpu.make_async_copy(cby.at[0], cby.at[0], cn_recv).wait()
    for m in range(1, half_ns):
        remote(cby.at[0], cby.at[m], cy_send, cy_recv, peer_shot(m))
    relay(far[0])
    peers = cby.at[pl.ds(1, half_ns - 1)]
    pltpu.make_async_copy(peers, peers, cy_recv).wait()
    half_corners = pltpu.make_async_copy(cby, csy, c_local.at[0])
    half_corners.start()
    pltpu.make_async_copy(cbuf, cbuf, c_recv).wait()
    all_corners = pltpu.make_async_copy(cbuf, csm, c_local.at[1])
    all_corners.start()
    half_corners.wait()
    all_corners.wait()

    gather_half(far[0])
    for u in far[1:]:
        relay(u)
    gather_whole(0)
    cross(0)
    stage2(0)
    for n in range(1, nb):
        gather_half(far[n])
    relay(own[0])
    gather_whole(1)
    for n in range(1, nb):
        cross(n)
    for u in own[1:]:
        relay(u)
    stage2(1)
    finish_whole(0)
    for u in own[:-1]:
        gather_half(u)
    finish_whole(1)
    gather_half(own[nb - 1])
    for n in range(nb - 1):
        finish_half(n)
    known = whole + middle
    for p in known:
        base_plane(p, known)
    finish_half(nb - 1)
    for p in near_planes(last):
        out[p] = out[p] + nrm[last]
    base_plane(last, known)

    for d in range(2):
        @pl.when(edges[d][0])
        def _(d=d):
            for p in whole:
                edge_copy(d, p).wait_send()

        @pl.when(faces[d][0])
        def _(d=d):
            face_copy(d).wait_send()

    def drain(ref, sem):
        pltpu.make_async_copy(ref, ref, sem).wait()

    drain(cbuf.at[pl.ds(0, nt - 1)], c_send)
    drain(cby.at[0, pl.ds(0, half_nt - 1)], cn_send)
    drain(cby.at[pl.ds(1, half_ns - 1)], cy_send)
    for u in range(len(whole)):
        drain(rxw.at[u, pl.ds(0, nt - 1)], rxw_send.at[u])
        drain(r1.at[u], s1_send.at[u])
        drain(r2.at[u], s2_send.at[u])
    for u in range(2 * nb):
        drain(rxh.at[u, 0, pl.ds(0, half_nt - 1)], rxh_send.at[u])
        drain(rxh.at[u, pl.ds(1, half_ns - 1)], ry_send.at[u])
        drain(hr1.at[u], h1_send.at[u, 0])
        drain(hal1.at[u], h1_send.at[u, 1])
    for n in range(nb):
        for copy in cross_copies(n):
            copy.wait_send()


def solution(mesh):
    ns, nt = mesh.shape["shot"], mesh.shape["tile"]

    def step(source, receiver, corners):
        spd, samples, full_depth, box_rows, box_cols = source.shape
        depth = full_depth // nt
        strip = X // ns
        block = min(box_rows, strip)
        half_ns = ns // 2
        half_nt = nt // 2
        whole, split = plan(depth)
        nw, nb = len(whole), len(split)
        vmem = pltpu.VMEM
        dma = pltpu.SemaphoreType.DMA
        f32 = jnp.float32
        bf16 = jnp.bfloat16
        waves = (2, spd, samples, box_rows, box_cols)
        return pl.pallas_call(
            functools.partial(kernel, ns, nt),
            out_shape=jax.ShapeDtypeStruct((depth, strip, Y), f32),
            in_specs=[pl.BlockSpec(memory_space=pl.ANY)] * 3,
            out_specs=pl.BlockSpec(memory_space=pltpu.VMEM),
            scratch_shapes=[
                vmem((full_depth, *waves), bf16),
                vmem((nw, nt, *waves), bf16),
                vmem((2 * nb, half_ns, half_nt, *waves), bf16),
                vmem((nt, spd, 2), jnp.int32),
                pltpu.SMEM((nt, spd, 2), jnp.int32),
                vmem((half_ns, half_nt, spd, 2), jnp.int32),
                pltpu.SMEM((half_ns, half_nt, spd, 2), jnp.int32),
                vmem((max(nt, half_ns * half_nt) * spd, 2, Y // LANES, box_rows + 2 * block, LANES), f32),
                vmem((nw, ns, 2, strip, Y), f32),
                vmem((nw, half_ns, 2, strip, Y), f32),
                vmem((nw, half_ns - 1, 2, strip, Y), f32),
                vmem((2 * nb, 2, 2, strip, Y), f32),
                vmem((2 * nb, 2, strip, Y), f32),
                vmem((2 * nb, 2, 4, Y), f32),
                vmem((2 * nb, 4, Y), f32),
                vmem((nb, 2, strip, Y), f32),
                vmem((nb, 2, strip, Y), f32),
                vmem((nb, 4, Y), f32),
                vmem((nb, 4, Y), f32),
                vmem((depth, strip, Y), f32),
                vmem((2, depth, 1, Y), f32),
                vmem((2, strip, Y), f32),
                vmem((2, depth, 1, Y), f32),
                dma,
                dma((nw,)),
                dma((nw,)),
                dma((2 * nb,)),
                dma((2 * nb, half_nt)),
                dma((2 * nb,)),
                dma((2 * nb,)),
                dma,
                dma,
                dma,
                dma,
                dma,
                dma,
                dma((2,)),
                dma((nw,)),
                dma((nw,)),
                dma((nw,)),
                dma((nw,)),
                dma((2 * nb, 2)),
                dma((2 * nb, 2)),
                dma((nb, 2)),
                dma((nb, 2)),
                dma((2, depth)),
                dma((2, depth)),
                dma((2,)),
                dma((2,)),
                pltpu.SemaphoreType.REGULAR((nt // 2 - 1,)),
            ],
            compiler_params=pltpu.CompilerParams(
                collective_id=0, has_side_effects=True, vmem_limit_bytes=54700 * 1024
            ),
        )(source, receiver, corners)

    return jax.shard_map(
        step,
        mesh=mesh,
        in_specs=(
            P(("shot", "tile"), None, None, None, None),
            P(("shot", "tile"), None, None, None, None),
            P(("shot", "tile"), None),
        ),
        out_specs=P("tile", "shot", None),
        check_vma=False,
    )
```

```python
import functools

import jax
import jax.numpy as jnp
from jax import lax
from jax.experimental import pallas as pl
from jax.experimental.pallas import tpu as pltpu
from jax.sharding import PartitionSpec as P

X = 256
Y = 256
LANES = 128

damping = 1.0


def partner(index, k, count):
    if count & (count - 1):
        return lax.rem(index + k, count)
    bit = 1
    result = index
    while bit < count:
        if k & bit:
            result = result + bit * (1 - 2 * lax.rem(index // bit, 2))
        bit *= 2
    return result


def partner_back(index, k, count):
    if count & (count - 1):
        return lax.rem(index + count - k, count)
    return partner(index, k, count)


def plan(depth):
    if depth < 3:
        return list(range(depth)), []
    return [0, depth - 1], list(range(1, depth - 1))


def kernel(
    ns, nt, src, rcv, cor, out, sbuf, rxw, rxh, cbuf, csm, cby, csy, boxes,
    acc, r1, r2, hacc, hr1, hal, hal1, mbuf, mx, mhal, mhx, nrm, hx, hz, rows,
    in_sem, rxw_send, rxw_recv, rxh_send, rxh_recv, ry_send, ry_recv,
    c_send, c_recv, cn_send, cn_recv, cy_send, cy_recv, c_local,
    s1_send, s1_recv, s2_send, s2_recv, h1_send, h1_recv, m_send, m_recv,
    row_send, row_recv, face_send, face_recv, known_sem,
):
    depth, strip, width = nrm.shape
    spd, samples = src.shape[0], src.shape[1]
    box_rows = src.shape[3]
    halves = width // LANES
    whole, split = plan(depth)
    block = min(box_rows, strip)
    per_strip = strip // block
    half_ns = ns // 2
    half_nt = nt // 2
    shot = lax.axis_index("shot")
    tile = lax.axis_index("tile")
    core = lax.rem(shot, 2)
    pair = shot // 2
    other = 1 - core
    mine = lax.rem(tile, half_nt)
    base = tile - mine
    mirror = lax.rem(tile + half_nt, nt)
    twin = {"shot": 2 * pair + other}
    nb = len(split)
    far = range(nb)
    own = range(nb, 2 * nb)
    plane = split + split

    def peer_shot(m):
        return {"shot": 2 * lax.rem(pair + m, half_ns) + core}

    def slab_of(u, to):
        return lax.rem(to + half_nt, nt) if u in far else to

    barrier = pltpu.get_barrier_semaphore()
    for k in range(1, ns):
        pl.semaphore_signal(barrier, inc=1, device_id={"shot": lax.rem(shot + k, ns)})
    column, side = tile // 2, lax.rem(tile, 2)
    columns = nt // 2
    around = (
        (None, {"tile": tile + 1 - 2 * side}),
        (column > 0, {"tile": lax.rem(tile + nt - 2, nt)}),
        (column < columns - 1, {"tile": lax.rem(tile + 2, nt)}),
    )

    def greet(sem):
        for there, who in around:
            if there is None:
                pl.semaphore_signal(sem, inc=1, device_id=who)
            else:
                @pl.when(there)
                def _(who=who):
                    pl.semaphore_signal(sem, inc=1, device_id=who)

    def await_greetings(sem, more):
        pl.semaphore_wait(sem, more + 1 + jnp.minimum(column, 1) + jnp.minimum(columns - 1 - column, 1))

    def learn(r):
        await_greetings(known_sem.at[r], 0)
        if r + 1 < known_sem.shape[0]:
            greet(known_sem.at[r + 1])

    greet(barrier)

    for w, ref in enumerate((src, rcv)):
        for i in range(spd):
            for n in range(samples):
                pltpu.make_async_copy(ref.at[i, n], sbuf.at[:, w, i, n], in_sem).start()
    pltpu.make_async_copy(cor, cbuf.at[tile], c_recv).start()
    pltpu.make_async_copy(cor, cby.at[0, mine], cn_recv).start()
    for w, ref in enumerate((src, rcv)):
        for u, p in enumerate(plane):
            pltpu.make_async_copy(
                ref.at[:, :, slab_of(u, tile) * depth + p], rxh.at[u, 0, mine, w], rxh_recv.at[u, 0]
            ).start()
        for u, p in enumerate(whole):
            pltpu.make_async_copy(ref.at[:, :, tile * depth + p], rxw.at[u, tile, w], rxw_recv.at[u]).start()
    pltpu.make_async_copy(sbuf, sbuf, in_sem).wait()

    await_greetings(barrier, ns - 1)
    greet(known_sem.at[0])

    def remote(src_ref, dst_ref, send_sem, recv_sem, device_id):
        pltpu.make_async_remote_copy(
            src_ref=src_ref, dst_ref=dst_ref, send_sem=send_sem, recv_sem=recv_sem, device_id=device_id
        ).start()

    def steps(to):
        return abs(to // 2 - column) + abs(lax.rem(to, 2) - side)

    def near_half(u, when=None, first=1, stop=half_nt):
        for k in range(first, stop):
            to = base + partner(mine, k, half_nt)
            guarded(when, to, lambda k=k, to=to: remote(
                sbuf.at[slab_of(u, to) * depth + plane[u]], rxh.at[u, 0, mine],
                rxh_send.at[u], rxh_recv.at[u, k], {"tile": to},
            ))

    def guarded(when, to, send):
        if when is None:
            send()
        else:
            @pl.when(when(steps(to)))
            def _():
                send()

    def own_half(u):
        for m in range(1, half_ns):
            remote(
                sbuf.at[slab_of(u, tile) * depth + plane[u]], rxh.at[u, m, mine],
                ry_send.at[u], ry_recv.at[u], peer_shot(m),
            )

    def relay(u, first=1, stop=half_nt):
        for k in range(first, stop):
            slot = partner_back(mine, k, half_nt)
            got = rxh.at[u, 0, slot]
            pltpu.make_async_copy(got, got, rxh_recv.at[u, k]).wait()
            for m in range(1, half_ns):
                remote(got, rxh.at[u, m, slot], ry_send.at[u], ry_recv.at[u], peer_shot(m))

    def near_whole(u, when=None):
        for k in range(1, half_nt):
            to = base + partner(mine, k, half_nt)
            guarded(when, to, lambda to=to: remote(
                sbuf.at[to * depth + whole[u]], rxw.at[u, tile], rxw_send.at[u], rxw_recv.at[u], {"tile": to}
            ))

    def far_whole(u, when=None):
        for k in range(half_nt):
            to = (half_nt - base) + partner(mine, k, half_nt)
            guarded(when, to, lambda to=to: remote(
                sbuf.at[to * depth + whole[u]], rxw.at[u, tile], rxw_send.at[u], rxw_recv.at[u], {"tile": to}
            ))

    def corners(when):
        for k in range(1, half_nt):
            to = base + partner(mine, k, half_nt)
            guarded(when, to, lambda to=to: remote(cor, cby.at[0, mine], cn_send, cn_recv, {"tile": to}))
        for k in range(1, nt):
            to = partner(tile, k, nt)
            guarded(when, to, lambda to=to: remote(cor, cbuf.at[tile], c_send, c_recv, {"tile": to}))

    for level in (1, 2, 3):
        if level == 1:
            when = lambda d: d == 1
        elif level == 2:
            learn(0)
            when = lambda d: d == 2
        else:
            for r in range(1, known_sem.shape[0]):
                learn(r)
            when = lambda d: d > 2
        corners(when)
        near_half(far[0], when)
        far_whole(0, when)
        if level == 1:
            for u in range(2 * nb):
                own_half(u)
            for u in own:
                near_half(u, None, 1, 2)
        near_whole(0, when)
    for u in far[1:]:
        near_half(u)
    far_whole(1)
    near_whole(1)
    for u in own:
        near_half(u, None, 2)

    edges = (
        (shot < ns - 1, shot > 0, {"shot": lax.rem(shot + 1, ns)}),
        (shot > 0, shot < ns - 1, {"shot": lax.rem(shot + ns - 1, ns)}),
    )
    faces = (
        (tile < nt - 1, tile > 0, {"tile": lax.rem(tile + 1, nt)}, depth - 1),
        (tile > 0, tile < nt - 1, {"tile": lax.rem(tile + nt - 1, nt)}, 0),
    )
    for d in range(2):
        @pl.when(jnp.logical_not(edges[d][1]))
        def _(d=d):
            hx[d] = jnp.zeros((depth, 1, width), jnp.float32)

        @pl.when(jnp.logical_not(faces[d][1]))
        def _(d=d):
            hz[d] = jnp.zeros((strip, width), jnp.float32)

    def edge_copy(d, p):
        return pltpu.make_async_remote_copy(
            src_ref=rows.at[d, p], dst_ref=hx.at[d, p],
            send_sem=row_send.at[d, p], recv_sem=row_recv.at[d, p], device_id=edges[d][2],
        )

    def face_copy(d):
        return pltpu.make_async_remote_copy(
            src_ref=nrm.at[faces[d][3]], dst_ref=hz.at[d],
            send_sem=face_send.at[d], recv_sem=face_recv.at[d], device_id=faces[d][2],
        )

    def cross_copies(n):
        pieces = []
        for g, (a, b) in enumerate(((mbuf, mx), (mhal, mhx))):
            pieces.append(pltpu.make_async_remote_copy(
                src_ref=a.at[n], dst_ref=b.at[n],
                send_sem=m_send.at[n, g], recv_sem=m_recv.at[n, g], device_id={"tile": mirror},
            ))
        return pieces

    zero = jnp.zeros((block, LANES), jnp.float32)

    def clear(s, carry):
        for q in range(2):
            for h in range(halves):
                boxes[s, q, h, pl.ds(0, block), :] = zero
                boxes[s, q, h, pl.ds(block + box_rows, block), :] = zero
        return carry

    lax.fori_loop(0, boxes.shape[0], clear, 0)

    lane = lax.broadcasted_iota(jnp.int32, (box_rows, LANES), 1)

    def expand_one(s, col, wave_of, back_of):
        turn = lax.rem(col, LANES)
        image = jnp.zeros((box_rows, LANES), jnp.float32)
        light = image
        for n in range(samples):
            wave = wave_of(n).astype(jnp.float32)
            back = back_of(n).astype(jnp.float32)
            image = wave * back if n == 0 else image + wave * back
            light = wave * wave if n == 0 else light + wave * wave
        image = pltpu.roll(image, turn, 1)
        light = pltpu.roll(light, turn, 1)
        for h in range(halves):
            at = lane + (h * LANES - col)
            inside = (at >= 0) & (at < LANES)
            boxes[s, 0, h, pl.ds(block, box_rows), :] = jnp.where(inside, image, 0.0)
            boxes[s, 1, h, pl.ds(block, box_rows), :] = jnp.where(inside, light, 0.0)

    def expand_whole(u):
        def peer(t, carry):
            for i in range(spd):
                expand_one(
                    t * spd + i, csm[t, i, 1],
                    lambda n: rxw[u, t, 0, i, n], lambda n: rxw[u, t, 1, i, n],
                )
            return carry

        lax.fori_loop(0, nt, peer, 0)

    def expand_half(u, first, stop):
        for m in range(first, stop):
            def peer(t, carry):
                for i in range(spd):
                    expand_one(
                        (m * half_nt + t) * spd + i, csy[m, t, i, 1],
                        lambda n: rxh[u, m, t, 0, i, n], lambda n: rxh[u, m, t, 1, i, n],
                    )
                return carry

            lax.fori_loop(0, half_nt, peer, 0)

    whole_rows = [(s, lambda s=s: csm[s // spd, s % spd, 0]) for s in range(nt * spd)]
    half_rows = [
        ((m * half_nt + t) * spd + i, lambda m=m, t=t, i=i: csy[m, t, i, 0])
        for m in range(half_ns) for t in range(half_nt) for i in range(spd)
    ]

    def stack(corner_rows, first, count):
        total = [[None] * halves for _ in range(2)]
        for s, corner in corner_rows:
            start = jnp.clip(first + block - corner(), 0, box_rows + block)
            for q in range(2):
                for h in range(halves):
                    piece = boxes[s, q, h, pl.ds(start, count), :]
                    total[q][h] = piece if total[q][h] is None else total[q][h] + piece
        return total

    def place_whole(u, parity):
        def one(n, carry):
            j = 2 * (n // per_strip) + parity
            at = lax.rem(n, per_strip) * block
            total = stack(whole_rows, j * strip + at, block)
            for q in range(2):
                for h in range(halves):
                    acc[u, j, q, pl.ds(at, block), pl.ds(h * LANES, LANES)] = total[q][h]
            return carry

        lax.fori_loop(0, half_ns * per_strip, one, 0)

    def place_half(u, parity):
        top = (2 * pair + parity) * strip

        def one(n, carry):
            at = n * block
            total = stack(half_rows, top + at, block)
            for q in range(2):
                for h in range(halves):
                    hacc[u, parity, q, pl.ds(at, block), pl.ds(h * LANES, LANES)] = total[q][h]
            return carry

        lax.fori_loop(0, per_strip, one, 0)
        for d, first in enumerate((top - 1, top + strip)):
            total = stack(half_rows, first, 1)
            for q in range(2):
                for h in range(halves):
                    hal[u, parity, pl.ds(2 * q + d, 1), pl.ds(h * LANES, LANES)] = total[q][h]

    def gather_whole(u):
        pltpu.make_async_copy(rxw.at[u], rxw.at[u], rxw_recv.at[u]).wait()
        expand_whole(u)
        place_whole(u, other)
        for i in range(half_ns):
            remote(acc.at[u, 2 * i + other], r1.at[u, i], s1_send.at[u], s1_recv.at[u], twin)
        place_whole(u, core)

    def gather_half(u):
        got = rxh.at[u, 0, mine]
        pltpu.make_async_copy(got, got, rxh_recv.at[u, 0]).wait()
        expand_half(u, 0, 1)
        got = rxh.at[u, pl.ds(1, half_ns - 1)]
        pltpu.make_async_copy(got, got, ry_recv.at[u]).wait()
        expand_half(u, 1, half_ns)
        place_half(u, other)
        remote(hacc.at[u, other], hr1.at[u], h1_send.at[u, 0], h1_recv.at[u, 0], twin)
        remote(hal.at[u, other], hal1.at[u], h1_send.at[u, 1], h1_recv.at[u, 1], twin)
        place_half(u, core)

    def wait_twin(u):
        pltpu.make_async_copy(hr1.at[u], hr1.at[u], h1_recv.at[u, 0]).wait()
        pltpu.make_async_copy(hal1.at[u], hal1.at[u], h1_recv.at[u, 1]).wait()

    def stage2(u):
        pltpu.make_async_copy(r1.at[u], r1.at[u], s1_recv.at[u]).wait()
        for k in range(1, half_ns):
            to = lax.rem(pair + k, half_ns)
            j = 2 * to + core
            acc[u, j] = acc[u, j] + r1[u, to]
            remote(acc.at[u, j], r2.at[u, k - 1], s2_send.at[u], s2_recv.at[u], {"shot": j})

    def cross(n):
        u = far[n]
        wait_twin(u)
        mhal[n] = hal[u, core] + hal1[u]
        mbuf[n] = hacc[u, core] + hr1[u]
        for copy in reversed(cross_copies(n)):
            copy.start()

    def finish_whole(u):
        p = whole[u]
        pltpu.make_async_copy(r2.at[u], r2.at[u], s2_recv.at[u]).wait()
        image = acc[u, shot, 0] + r1[u, pair, 0]
        light = acc[u, shot, 1] + r1[u, pair, 1]
        for k in range(half_ns - 1):
            image = image + r2[u, k, 0]
            light = light + r2[u, k, 1]
        normal = image / (damping + light)
        nrm[p] = normal
        rows[0, p] = normal[strip - 1 :, :]
        rows[1, p] = normal[:1, :]
        for d in range(2):
            @pl.when(edges[d][0])
            def _(d=d):
                edge_copy(d, p).start()

            if p == faces[d][3]:
                @pl.when(faces[d][0])
                def _(d=d):
                    face_copy(d).start()

    def finish_half(n):
        p, u = split[n], own[n]
        wait_twin(u)
        for copy in cross_copies(n):
            copy.wait_recv()
        image = (hacc[u, core, 0] + hr1[u, 0]) + mx[n, 0]
        light = (hacc[u, core, 1] + hr1[u, 1]) + mx[n, 1]
        nrm[p] = image / (damping + light)
        rim = hal[u, core] + hal1[u] + mhx[n]
        rim = rim[0:2, :] / (damping + rim[2:4, :])
        hx[0, p] = rim[0:1, :]
        hx[1, p] = rim[1:2, :]

    row = lax.broadcasted_iota(jnp.int32, (strip, width), 0)
    lanes = lax.broadcasted_iota(jnp.int32, (strip, width), 1)

    def lateral(p):
        center = nrm[p]
        before = jnp.where(row == 0, hx[0, p], pltpu.roll(center, 1, 0))
        after = jnp.where(row == strip - 1, hx[1, p], pltpu.roll(center, strip - 1, 0))
        left = jnp.where(lanes == 0, 0.0, pltpu.roll(center, 1, 1))
        right = jnp.where(lanes == width - 1, 0.0, pltpu.roll(center, width - 1, 1))
        return before + after + left + right - 6.0 * center

    def near_planes(p):
        return [q for q in (p - 1, p + 1) if 0 <= q < depth]

    def base_plane(p, known):
        if p in whole:
            for d in range(2):
                @pl.when(edges[d][1])
                def _(d=d):
                    edge_copy(d, p).wait_recv()
        value = lateral(p)
        for q in near_planes(p):
            if q in known:
                value = value + nrm[q]
        for d in range(2):
            if p == (depth - 1 if d else 0):
                @pl.when(faces[d][1])
                def _(d=d):
                    face_copy(d).wait_recv()
                value = value + hz[d]
        out[p] = value

    last = split[-1]
    middle = split[:-1]

    pltpu.make_async_copy(cby.at[0], cby.at[0], cn_recv).wait()
    for m in range(1, half_ns):
        remote(cby.at[0], cby.at[m], cy_send, cy_recv, peer_shot(m))
    relay(far[0])
    peers = cby.at[pl.ds(1, half_ns - 1)]
    pltpu.make_async_copy(peers, peers, cy_recv).wait()
    half_corners = pltpu.make_async_copy(cby, csy, c_local.at[0])
    half_corners.start()
    for u in own:
        relay(u, 1, 2)
    half_corners.wait()

    gather_half(far[0])
    pltpu.make_async_copy(cbuf, cbuf, c_recv).wait()
    all_corners = pltpu.make_async_copy(cbuf, csm, c_local.at[1])
    all_corners.start()
    for u in far[1:]:
        relay(u)
    all_corners.wait()
    gather_whole(0)
    cross(0)
    stage2(0)
    for n in range(1, nb):
        gather_half(far[n])
        cross(n)
    gather_whole(1)
    relay(own[0], 2)
    stage2(1)
    for u in own[1:]:
        relay(u, 2)
    finish_whole(0)
    for u in own[:-1]:
        gather_half(u)
    finish_whole(1)
    gather_half(own[nb - 1])
    for n in range(nb - 1):
        finish_half(n)
    known = whole + middle
    for p in known:
        base_plane(p, known)
    finish_half(nb - 1)
    for p in near_planes(last):
        out[p] = out[p] + nrm[last]
    base_plane(last, known)

    for d in range(2):
        @pl.when(edges[d][0])
        def _(d=d):
            for p in whole:
                edge_copy(d, p).wait_send()

        @pl.when(faces[d][0])
        def _(d=d):
            face_copy(d).wait_send()

    def drain(ref, sem):
        pltpu.make_async_copy(ref, ref, sem).wait()

    drain(cbuf.at[pl.ds(0, nt - 1)], c_send)
    drain(cby.at[0, pl.ds(0, half_nt - 1)], cn_send)
    drain(cby.at[pl.ds(1, half_ns - 1)], cy_send)
    for u in range(len(whole)):
        drain(rxw.at[u, pl.ds(0, nt - 1)], rxw_send.at[u])
        drain(r1.at[u], s1_send.at[u])
        drain(r2.at[u], s2_send.at[u])
    for u in range(2 * nb):
        drain(rxh.at[u, 0, pl.ds(0, half_nt - 1)], rxh_send.at[u])
        drain(rxh.at[u, pl.ds(1, half_ns - 1)], ry_send.at[u])
        drain(hr1.at[u], h1_send.at[u, 0])
        drain(hal1.at[u], h1_send.at[u, 1])
    for n in range(nb):
        for copy in cross_copies(n):
            copy.wait_send()


def solution(mesh):
    ns, nt = mesh.shape["shot"], mesh.shape["tile"]

    def step(source, receiver, corners):
        spd, samples, full_depth, box_rows, box_cols = source.shape
        depth = full_depth // nt
        strip = X // ns
        block = min(box_rows, strip)
        half_ns = ns // 2
        half_nt = nt // 2
        whole, split = plan(depth)
        nw, nb = len(whole), len(split)
        vmem = pltpu.VMEM
        dma = pltpu.SemaphoreType.DMA
        f32 = jnp.float32
        bf16 = jnp.bfloat16
        waves = (2, spd, samples, box_rows, box_cols)
        return pl.pallas_call(
            functools.partial(kernel, ns, nt),
            out_shape=jax.ShapeDtypeStruct((depth, strip, Y), f32),
            in_specs=[pl.BlockSpec(memory_space=pl.ANY)] * 3,
            out_specs=pl.BlockSpec(memory_space=pltpu.VMEM),
            scratch_shapes=[
                vmem((full_depth, *waves), bf16),
                vmem((nw, nt, *waves), bf16),
                vmem((2 * nb, half_ns, half_nt, *waves), bf16),
                vmem((nt, spd, 2), jnp.int32),
                pltpu.SMEM((nt, spd, 2), jnp.int32),
                vmem((half_ns, half_nt, spd, 2), jnp.int32),
                pltpu.SMEM((half_ns, half_nt, spd, 2), jnp.int32),
                vmem((max(nt, half_ns * half_nt) * spd, 2, Y // LANES, box_rows + 2 * block, LANES), f32),
                vmem((nw, ns, 2, strip, Y), f32),
                vmem((nw, half_ns, 2, strip, Y), f32),
                vmem((nw, half_ns - 1, 2, strip, Y), f32),
                vmem((2 * nb, 2, 2, strip, Y), f32),
                vmem((2 * nb, 2, strip, Y), f32),
                vmem((2 * nb, 2, 4, Y), f32),
                vmem((2 * nb, 4, Y), f32),
                vmem((nb, 2, strip, Y), f32),
                vmem((nb, 2, strip, Y), f32),
                vmem((nb, 4, Y), f32),
                vmem((nb, 4, Y), f32),
                vmem((depth, strip, Y), f32),
                vmem((2, depth, 1, Y), f32),
                vmem((2, strip, Y), f32),
                vmem((2, depth, 1, Y), f32),
                dma,
                dma((nw,)),
                dma((nw,)),
                dma((2 * nb,)),
                dma((2 * nb, half_nt)),
                dma((2 * nb,)),
                dma((2 * nb,)),
                dma,
                dma,
                dma,
                dma,
                dma,
                dma,
                dma((2,)),
                dma((nw,)),
                dma((nw,)),
                dma((nw,)),
                dma((nw,)),
                dma((2 * nb, 2)),
                dma((2 * nb, 2)),
                dma((nb, 2)),
                dma((nb, 2)),
                dma((2, depth)),
                dma((2, depth)),
                dma((2,)),
                dma((2,)),
                pltpu.SemaphoreType.REGULAR((nt // 2 - 1,)),
            ],
            compiler_params=pltpu.CompilerParams(
                collective_id=0, has_side_effects=True, vmem_limit_bytes=54700 * 1024
            ),
        )(source, receiver, corners)

    return jax.shard_map(
        step,
        mesh=mesh,
        in_specs=(
            P(("shot", "tile"), None, None, None, None),
            P(("shot", "tile"), None, None, None, None),
            P(("shot", "tile"), None),
        ),
        out_specs=P("tile", "shot", None),
        check_vma=False,
    )
```

```python
import functools

import jax
import jax.numpy as jnp
from jax import lax
from jax.experimental import pallas as pl
from jax.experimental.pallas import tpu as pltpu
from jax.sharding import PartitionSpec as P

X = 256
Y = 256
LANES = 128

damping = 1.0


def partner(index, k, count):
    if count & (count - 1):
        return lax.rem(index + k, count)
    bit = 1
    result = index
    while bit < count:
        if k & bit:
            result = result + bit * (1 - 2 * lax.rem(index // bit, 2))
        bit *= 2
    return result


def partner_back(index, k, count):
    if count & (count - 1):
        return lax.rem(index + count - k, count)
    return partner(index, k, count)


def plan(depth):
    if depth < 3:
        return list(range(depth)), []
    return [0, depth - 1], list(range(1, depth - 1))


def kernel(
    ns, nt, src, rcv, cor, out, sbuf, rxw, rxh, cbuf, csm, cby, csy, boxes,
    acc, r1, r2, hacc, hr1, hal, hal1, mbuf, mx, mhal, mhx, nrm, hx, hz, rows,
    in_sem, rxw_send, rxw_recv, rxh_send, rxh_recv, ry_send, ry_recv,
    c_send, c_recv, cn_send, cn_recv, cy_send, cy_recv, c_local,
    s1_send, s1_recv, s2_send, s2_recv, h1_send, h1_recv, m_send, m_recv,
    row_send, row_recv, face_send, face_recv, known_sem,
):
    depth, strip, width = nrm.shape
    spd, samples = src.shape[0], src.shape[1]
    box_rows = src.shape[3]
    halves = width // LANES
    whole, split = plan(depth)
    block = min(box_rows, strip)
    per_strip = strip // block
    half_ns = ns // 2
    half_nt = nt // 2
    shot = lax.axis_index("shot")
    tile = lax.axis_index("tile")
    core = lax.rem(shot, 2)
    pair = shot // 2
    other = 1 - core
    mine = lax.rem(tile, half_nt)
    base = tile - mine
    mirror = lax.rem(tile + half_nt, nt)
    twin = {"shot": 2 * pair + other}
    nb = len(split)
    far = range(nb)
    own = range(nb, 2 * nb)
    plane = split + split

    def peer_shot(m):
        return {"shot": 2 * lax.rem(pair + m, half_ns) + core}

    def slab_of(u, to):
        return lax.rem(to + half_nt, nt) if u in far else to

    barrier = pltpu.get_barrier_semaphore()
    for k in range(1, ns):
        pl.semaphore_signal(barrier, inc=1, device_id={"shot": lax.rem(shot + k, ns)})
    column, side = tile // 2, lax.rem(tile, 2)
    columns = nt // 2
    around = (
        (None, {"tile": tile + 1 - 2 * side}),
        (column > 0, {"tile": lax.rem(tile + nt - 2, nt)}),
        (column < columns - 1, {"tile": lax.rem(tile + 2, nt)}),
    )

    def greet(sem):
        for there, who in around:
            if there is None:
                pl.semaphore_signal(sem, inc=1, device_id=who)
            else:
                @pl.when(there)
                def _(who=who):
                    pl.semaphore_signal(sem, inc=1, device_id=who)

    def await_greetings(sem, more):
        pl.semaphore_wait(sem, more + 1 + jnp.minimum(column, 1) + jnp.minimum(columns - 1 - column, 1))

    def learn(r):
        await_greetings(known_sem.at[r], 0)
        if r + 1 < known_sem.shape[0]:
            greet(known_sem.at[r + 1])

    greet(barrier)

    for w, ref in enumerate((src, rcv)):
        for i in range(spd):
            for n in range(samples):
                pltpu.make_async_copy(ref.at[i, n], sbuf.at[:, w, i, n], in_sem).start()
    pltpu.make_async_copy(cor, cbuf.at[tile], c_recv).start()
    pltpu.make_async_copy(cor, cby.at[0, mine], cn_recv).start()
    for w, ref in enumerate((src, rcv)):
        for u, p in enumerate(plane):
            pltpu.make_async_copy(
                ref.at[:, :, slab_of(u, tile) * depth + p], rxh.at[u, 0, mine, w], rxh_recv.at[u, 0]
            ).start()
        for u, p in enumerate(whole):
            pltpu.make_async_copy(ref.at[:, :, tile * depth + p], rxw.at[u, tile, w], rxw_recv.at[u]).start()

    await_greetings(barrier, ns - 1)
    greet(known_sem.at[0])
    pltpu.make_async_copy(sbuf, sbuf, in_sem).wait()

    def remote(src_ref, dst_ref, send_sem, recv_sem, device_id):
        pltpu.make_async_remote_copy(
            src_ref=src_ref, dst_ref=dst_ref, send_sem=send_sem, recv_sem=recv_sem, device_id=device_id
        ).start()

    def steps(to):
        return abs(to // 2 - column) + abs(lax.rem(to, 2) - side)

    def near_half(u, when=None, first=1, stop=half_nt):
        for k in range(first, stop):
            to = base + partner(mine, k, half_nt)
            guarded(when, to, lambda k=k, to=to: remote(
                sbuf.at[slab_of(u, to) * depth + plane[u]], rxh.at[u, 0, mine],
                rxh_send.at[u], rxh_recv.at[u, k], {"tile": to},
            ))

    def guarded(when, to, send):
        if when is None:
            send()
        else:
            @pl.when(when(steps(to)))
            def _():
                send()

    def own_half(u):
        for m in range(1, half_ns):
            remote(
                sbuf.at[slab_of(u, tile) * depth + plane[u]], rxh.at[u, m, mine],
                ry_send.at[u], ry_recv.at[u], peer_shot(m),
            )

    def relay(u, first=1, stop=half_nt):
        for k in range(first, stop):
            slot = partner_back(mine, k, half_nt)
            got = rxh.at[u, 0, slot]
            pltpu.make_async_copy(got, got, rxh_recv.at[u, k]).wait()
            for m in range(1, half_ns):
                remote(got, rxh.at[u, m, slot], ry_send.at[u], ry_recv.at[u], peer_shot(m))

    def near_whole(u, when=None):
        for k in range(1, half_nt):
            to = base + partner(mine, k, half_nt)
            guarded(when, to, lambda to=to: remote(
                sbuf.at[to * depth + whole[u]], rxw.at[u, tile], rxw_send.at[u], rxw_recv.at[u], {"tile": to}
            ))

    def far_whole(u, when=None):
        for k in range(half_nt):
            to = (half_nt - base) + partner(mine, k, half_nt)
            guarded(when, to, lambda to=to: remote(
                sbuf.at[to * depth + whole[u]], rxw.at[u, tile], rxw_send.at[u], rxw_recv.at[u], {"tile": to}
            ))

    def corners(when):
        for k in range(1, half_nt):
            to = base + partner(mine, k, half_nt)
            guarded(when, to, lambda to=to: remote(cor, cby.at[0, mine], cn_send, cn_recv, {"tile": to}))
        for k in range(1, nt):
            to = partner(tile, k, nt)
            guarded(when, to, lambda to=to: remote(cor, cbuf.at[tile], c_send, c_recv, {"tile": to}))

    early = own

    def early_half(when):
        for u in early:
            near_half(u, when, 1, 2)

    for level in (1, 2, 3):
        if level == 1:
            when = lambda d: d == 1
        elif level == 2:
            learn(0)
            when = lambda d: d == 2
        else:
            for r in range(1, known_sem.shape[0]):
                learn(r)
            when = lambda d: d > 2
        corners(when)
        near_half(far[0], when)
        far_whole(0, when)
        if level == 1:
            for u in range(2 * nb):
                own_half(u)
        early_half(when)
        near_whole(0, when)
        if level in (1,):
            far_whole(1, when)
    for u in far[1:]:
        near_half(u, None, 1)
    far_whole(1, lambda d: d > 1)
    near_whole(1)
    for u in own:
        near_half(u, None, 2)

    edges = (
        (shot < ns - 1, shot > 0, {"shot": lax.rem(shot + 1, ns)}),
        (shot > 0, shot < ns - 1, {"shot": lax.rem(shot + ns - 1, ns)}),
    )
    faces = (
        (tile < nt - 1, tile > 0, {"tile": lax.rem(tile + 1, nt)}, depth - 1),
        (tile > 0, tile < nt - 1, {"tile": lax.rem(tile + nt - 1, nt)}, 0),
    )
    for d in range(2):
        @pl.when(jnp.logical_not(edges[d][1]))
        def _(d=d):
            hx[d] = jnp.zeros((depth, 1, width), jnp.float32)

    def edge_copy(d, p):
        return pltpu.make_async_remote_copy(
            src_ref=rows.at[d, p], dst_ref=hx.at[d, p],
            send_sem=row_send.at[d, p], recv_sem=row_recv.at[d, p], device_id=edges[d][2],
        )

    def face_copy(d):
        return pltpu.make_async_remote_copy(
            src_ref=nrm.at[faces[d][3]], dst_ref=hz.at[d],
            send_sem=face_send.at[d], recv_sem=face_recv.at[d], device_id=faces[d][2],
        )

    def cross_copies(n):
        pieces = []
        for g, (a, b) in enumerate(((mbuf, mx), (mhal, mhx))):
            pieces.append(pltpu.make_async_remote_copy(
                src_ref=a.at[n], dst_ref=b.at[n],
                send_sem=m_send.at[n, g], recv_sem=m_recv.at[n, g], device_id={"tile": mirror},
            ))
        return pieces

    zero = jnp.zeros((block, LANES), jnp.float32)

    def clear(s, carry):
        for q in range(2):
            for h in range(halves):
                boxes[s, q, h, pl.ds(0, block), :] = zero
                boxes[s, q, h, pl.ds(block + box_rows, block), :] = zero
        return carry

    lax.fori_loop(0, boxes.shape[0], clear, 0)

    lane = lax.broadcasted_iota(jnp.int32, (box_rows, LANES), 1)

    def expand_one(s, col, wave_of, back_of):
        turn = lax.rem(col, LANES)
        image = jnp.zeros((box_rows, LANES), jnp.float32)
        light = image
        for n in range(samples):
            wave = wave_of(n).astype(jnp.float32)
            back = back_of(n).astype(jnp.float32)
            image = wave * back if n == 0 else image + wave * back
            light = wave * wave if n == 0 else light + wave * wave
        image = pltpu.roll(image, turn, 1)
        light = pltpu.roll(light, turn, 1)
        for h in range(halves):
            at = lane + (h * LANES - col)
            inside = (at >= 0) & (at < LANES)
            boxes[s, 0, h, pl.ds(block, box_rows), :] = jnp.where(inside, image, 0.0)
            boxes[s, 1, h, pl.ds(block, box_rows), :] = jnp.where(inside, light, 0.0)

    def expand_whole(u):
        def peer(t, carry):
            for i in range(spd):
                expand_one(
                    t * spd + i, csm[t, i, 1],
                    lambda n: rxw[u, t, 0, i, n], lambda n: rxw[u, t, 1, i, n],
                )
            return carry

        lax.fori_loop(0, nt, peer, 0)

    def expand_half(u, first, stop):
        for m in range(first, stop):
            def peer(t, carry):
                for i in range(spd):
                    expand_one(
                        (m * half_nt + t) * spd + i, csy[m, t, i, 1],
                        lambda n: rxh[u, m, t, 0, i, n], lambda n: rxh[u, m, t, 1, i, n],
                    )
                return carry

            lax.fori_loop(0, half_nt, peer, 0)

    whole_rows = [(s, lambda s=s: csm[s // spd, s % spd, 0]) for s in range(nt * spd)]
    half_rows = [
        ((m * half_nt + t) * spd + i, lambda m=m, t=t, i=i: csy[m, t, i, 0])
        for m in range(half_ns) for t in range(half_nt) for i in range(spd)
    ]

    def stack(corner_rows, first, count):
        total = [[None] * halves for _ in range(2)]
        for s, corner in corner_rows:
            start = jnp.clip(first + block - corner(), 0, box_rows + block)
            for q in range(2):
                for h in range(halves):
                    piece = boxes[s, q, h, pl.ds(start, count), :]
                    total[q][h] = piece if total[q][h] is None else total[q][h] + piece
        return total

    def place_whole(u, parity):
        def one(n, carry):
            j = 2 * (n // per_strip) + parity
            at = lax.rem(n, per_strip) * block
            total = stack(whole_rows, j * strip + at, block)
            for q in range(2):
                for h in range(halves):
                    acc[u, j, q, pl.ds(at, block), pl.ds(h * LANES, LANES)] = total[q][h]
            return carry

        lax.fori_loop(0, half_ns * per_strip, one, 0)

    def place_half(u, parity):
        top = (2 * pair + parity) * strip

        def one(n, carry):
            at = n * block
            total = stack(half_rows, top + at, block)
            for q in range(2):
                for h in range(halves):
                    hacc[u, parity, q, pl.ds(at, block), pl.ds(h * LANES, LANES)] = total[q][h]
            return carry

        lax.fori_loop(0, per_strip, one, 0)
        for d, first in enumerate((top - 1, top + strip)):
            total = stack(half_rows, first, 1)
            for q in range(2):
                for h in range(halves):
                    hal[u, parity, pl.ds(2 * q + d, 1), pl.ds(h * LANES, LANES)] = total[q][h]

    def receive_whole(u):
        pltpu.make_async_copy(rxw.at[u], rxw.at[u], rxw_recv.at[u]).wait()
        expand_whole(u)

    def spread_whole(u):
        place_whole(u, other)
        for i in range(half_ns):
            remote(acc.at[u, 2 * i + other], r1.at[u, i], s1_send.at[u], s1_recv.at[u], twin)
        place_whole(u, core)

    def gather_whole(u):
        receive_whole(u)
        spread_whole(u)

    def gather_half(u):
        got = rxh.at[u, 0, mine]
        pltpu.make_async_copy(got, got, rxh_recv.at[u, 0]).wait()
        expand_half(u, 0, 1)
        got = rxh.at[u, pl.ds(1, half_ns - 1)]
        pltpu.make_async_copy(got, got, ry_recv.at[u]).wait()
        expand_half(u, 1, half_ns)
        place_half(u, other)
        remote(hacc.at[u, other], hr1.at[u], h1_send.at[u, 0], h1_recv.at[u, 0], twin)
        remote(hal.at[u, other], hal1.at[u], h1_send.at[u, 1], h1_recv.at[u, 1], twin)
        place_half(u, core)

    def wait_twin(u):
        pltpu.make_async_copy(hr1.at[u], hr1.at[u], h1_recv.at[u, 0]).wait()
        pltpu.make_async_copy(hal1.at[u], hal1.at[u], h1_recv.at[u, 1]).wait()

    def stage2(u):
        pltpu.make_async_copy(r1.at[u], r1.at[u], s1_recv.at[u]).wait()
        for k in range(1, half_ns):
            to = lax.rem(pair + k, half_ns)
            j = 2 * to + core
            acc[u, j] = acc[u, j] + r1[u, to]
            remote(acc.at[u, j], r2.at[u, k - 1], s2_send.at[u], s2_recv.at[u], {"shot": j})

    def cross(n):
        u = far[n]
        wait_twin(u)
        mhal[n] = hal[u, core] + hal1[u]
        mbuf[n] = hacc[u, core] + hr1[u]
        for copy in reversed(cross_copies(n)):
            copy.start()

    def finish_whole(u):
        p = whole[u]
        pltpu.make_async_copy(r2.at[u], r2.at[u], s2_recv.at[u]).wait()
        image = acc[u, shot, 0] + r1[u, pair, 0]
        light = acc[u, shot, 1] + r1[u, pair, 1]
        for k in range(half_ns - 1):
            image = image + r2[u, k, 0]
            light = light + r2[u, k, 1]
        normal = image / (damping + light)
        nrm[p] = normal
        rows[0, p] = normal[strip - 1 :, :]
        rows[1, p] = normal[:1, :]
        for d in range(2):
            @pl.when(edges[d][0])
            def _(d=d):
                edge_copy(d, p).start()

            if p == faces[d][3]:
                @pl.when(faces[d][0])
                def _(d=d):
                    face_copy(d).start()

    def finish_half(n):
        p, u = split[n], own[n]
        wait_twin(u)
        for copy in cross_copies(n):
            copy.wait_recv()
        image = (hacc[u, core, 0] + hr1[u, 0]) + mx[n, 0]
        light = (hacc[u, core, 1] + hr1[u, 1]) + mx[n, 1]
        nrm[p] = image / (damping + light)
        rim = hal[u, core] + hal1[u] + mhx[n]
        rim = rim[0:2, :] / (damping + rim[2:4, :])
        hx[0, p] = rim[0:1, :]
        hx[1, p] = rim[1:2, :]

    row = lax.broadcasted_iota(jnp.int32, (strip, width), 0)
    lanes = lax.broadcasted_iota(jnp.int32, (strip, width), 1)

    def lateral(p):
        center = nrm[p]
        above = 0.0 if p in whole else hx[0, p]
        below = 0.0 if p in whole else hx[1, p]
        before = jnp.where(row == 0, above, pltpu.roll(center, 1, 0))
        after = jnp.where(row == strip - 1, below, pltpu.roll(center, strip - 1, 0))
        left = jnp.where(lanes == 0, 0.0, pltpu.roll(center, 1, 1))
        right = jnp.where(lanes == width - 1, 0.0, pltpu.roll(center, width - 1, 1))
        return before + after + left + right - 6.0 * center

    def near_planes(p):
        return [q for q in (p - 1, p + 1) if 0 <= q < depth]

    def base_plane(p, known):
        value = lateral(p)
        for q in near_planes(p):
            if q in known:
                value = value + nrm[q]
        out[p] = value

    def add_outside():
        for p in whole:
            for d in range(2):
                @pl.when(edges[d][1])
                def _(d=d):
                    edge_copy(d, p).wait_recv()
            out[p, pl.ds(0, 1), :] = out[p, pl.ds(0, 1), :] + hx[0, p]
            out[p, pl.ds(strip - 1, 1), :] = out[p, pl.ds(strip - 1, 1), :] + hx[1, p]
        for d, p in ((0, 0), (1, depth - 1)):
            @pl.when(faces[d][1])
            def _(d=d, p=p):
                face_copy(d).wait_recv()
                out[p] = out[p] + hz[d]

    last = split[-1]
    middle = split[:-1]

    pltpu.make_async_copy(cby.at[0], cby.at[0], cn_recv).wait()
    for m in range(1, half_ns):
        remote(cby.at[0], cby.at[m], cy_send, cy_recv, peer_shot(m))
    relay(far[0])
    peers = cby.at[pl.ds(1, half_ns - 1)]
    pltpu.make_async_copy(peers, peers, cy_recv).wait()
    half_corners = pltpu.make_async_copy(cby, csy, c_local.at[0])
    half_corners.start()
    for u in early:
        relay(u, 1, 2)
    half_corners.wait()

    gather_half(far[0])
    pltpu.make_async_copy(cbuf, cbuf, c_recv).wait()
    all_corners = pltpu.make_async_copy(cbuf, csm, c_local.at[1])
    all_corners.start()
    for u in far[1:]:
        relay(u, 1)
    all_corners.wait()
    gather_whole(0)
    cross(0)
    stage2(0)
    for n in range(1, nb):
        gather_half(far[n])
    receive_whole(1)
    for n in range(1, nb):
        cross(n)
    spread_whole(1)
    relay(own[0], 2)
    stage2(1)
    for u in own[1:]:
        relay(u, 2)
    finish_whole(0)
    for u in own[:-1]:
        gather_half(u)
    finish_whole(1)
    gather_half(own[nb - 1])
    for n in range(nb - 1):
        finish_half(n)
    known = whole + middle
    for p in known:
        base_plane(p, known)
    finish_half(nb - 1)
    for p in near_planes(last):
        out[p] = out[p] + nrm[last]
    base_plane(last, known)
    add_outside()

    for d in range(2):
        @pl.when(edges[d][0])
        def _(d=d):
            for p in whole:
                edge_copy(d, p).wait_send()

        @pl.when(faces[d][0])
        def _(d=d):
            face_copy(d).wait_send()

    def drain(ref, sem):
        pltpu.make_async_copy(ref, ref, sem).wait()

    drain(cbuf.at[pl.ds(0, nt - 1)], c_send)
    drain(cby.at[0, pl.ds(0, half_nt - 1)], cn_send)
    drain(cby.at[pl.ds(1, half_ns - 1)], cy_send)
    for u in range(len(whole)):
        drain(rxw.at[u, pl.ds(0, nt - 1)], rxw_send.at[u])
        drain(r1.at[u], s1_send.at[u])
        drain(r2.at[u], s2_send.at[u])
    for u in range(2 * nb):
        drain(rxh.at[u, 0, pl.ds(0, half_nt - 1)], rxh_send.at[u])
        drain(rxh.at[u, pl.ds(1, half_ns - 1)], ry_send.at[u])
        drain(hr1.at[u], h1_send.at[u, 0])
        drain(hal1.at[u], h1_send.at[u, 1])
    for n in range(nb):
        for copy in cross_copies(n):
            copy.wait_send()


def solution(mesh):
    ns, nt = mesh.shape["shot"], mesh.shape["tile"]

    def step(source, receiver, corners):
        spd, samples, full_depth, box_rows, box_cols = source.shape
        depth = full_depth // nt
        strip = X // ns
        block = min(box_rows, strip)
        half_ns = ns // 2
        half_nt = nt // 2
        whole, split = plan(depth)
        nw, nb = len(whole), len(split)
        vmem = pltpu.VMEM
        dma = pltpu.SemaphoreType.DMA
        f32 = jnp.float32
        bf16 = jnp.bfloat16
        waves = (2, spd, samples, box_rows, box_cols)
        return pl.pallas_call(
            functools.partial(kernel, ns, nt),
            out_shape=jax.ShapeDtypeStruct((depth, strip, Y), f32),
            in_specs=[pl.BlockSpec(memory_space=pl.ANY)] * 3,
            out_specs=pl.BlockSpec(memory_space=pltpu.VMEM),
            scratch_shapes=[
                vmem((full_depth, *waves), bf16),
                vmem((nw, nt, *waves), bf16),
                vmem((2 * nb, half_ns, half_nt, *waves), bf16),
                vmem((nt, spd, 2), jnp.int32),
                pltpu.SMEM((nt, spd, 2), jnp.int32),
                vmem((half_ns, half_nt, spd, 2), jnp.int32),
                pltpu.SMEM((half_ns, half_nt, spd, 2), jnp.int32),
                vmem((max(nt, half_ns * half_nt) * spd, 2, Y // LANES, box_rows + 2 * block, LANES), f32),
                vmem((nw, ns, 2, strip, Y), f32),
                vmem((nw, half_ns, 2, strip, Y), f32),
                vmem((nw, half_ns - 1, 2, strip, Y), f32),
                vmem((2 * nb, 2, 2, strip, Y), f32),
                vmem((2 * nb, 2, strip, Y), f32),
                vmem((2 * nb, 2, 4, Y), f32),
                vmem((2 * nb, 4, Y), f32),
                vmem((nb, 2, strip, Y), f32),
                vmem((nb, 2, strip, Y), f32),
                vmem((nb, 4, Y), f32),
                vmem((nb, 4, Y), f32),
                vmem((depth, strip, Y), f32),
                vmem((2, depth, 1, Y), f32),
                vmem((2, strip, Y), f32),
                vmem((2, depth, 1, Y), f32),
                dma,
                dma((nw,)),
                dma((nw,)),
                dma((2 * nb,)),
                dma((2 * nb, half_nt)),
                dma((2 * nb,)),
                dma((2 * nb,)),
                dma,
                dma,
                dma,
                dma,
                dma,
                dma,
                dma((2,)),
                dma((nw,)),
                dma((nw,)),
                dma((nw,)),
                dma((nw,)),
                dma((2 * nb, 2)),
                dma((2 * nb, 2)),
                dma((nb, 2)),
                dma((nb, 2)),
                dma((2, depth)),
                dma((2, depth)),
                dma((2,)),
                dma((2,)),
                pltpu.SemaphoreType.REGULAR((nt // 2 - 1,)),
            ],
            compiler_params=pltpu.CompilerParams(
                collective_id=0, has_side_effects=True, vmem_limit_bytes=54700 * 1024
            ),
        )(source, receiver, corners)

    return jax.shard_map(
        step,
        mesh=mesh,
        in_specs=(
            P(("shot", "tile"), None, None, None, None),
            P(("shot", "tile"), None, None, None, None),
            P(("shot", "tile"), None),
        ),
        out_specs=P("tile", "shot", None),
        check_vma=False,
    )
```

```python
import functools

import jax
import jax.numpy as jnp
from jax import lax
from jax.experimental import pallas as pl
from jax.experimental.pallas import tpu as pltpu
from jax.sharding import PartitionSpec as P

X = 256
Y = 256
LANES = 128

damping = 1.0


def partner(index, k, count):
    if count & (count - 1):
        return lax.rem(index + k, count)
    bit = 1
    result = index
    while bit < count:
        if k & bit:
            result = result + bit * (1 - 2 * lax.rem(index // bit, 2))
        bit *= 2
    return result


def partner_back(index, k, count):
    if count & (count - 1):
        return lax.rem(index + count - k, count)
    return partner(index, k, count)


def plan(depth):
    if depth < 3:
        return list(range(depth)), []
    return [0, depth - 1], list(range(1, depth - 1))


def kernel(
    ns, nt, src, rcv, cor, out, sbuf, rxw, rxh, cbuf, csm, cby, csy, boxes,
    acc, r1, r2, hacc, hr1, hal, hal1, mbuf, mx, mhal, mhx, nrm, hx, hz, rows,
    in_sem, rxw_send, rxw_recv, rxh_send, rxh_recv, ry_send, ry_recv,
    c_send, c_recv, cn_send, cn_recv, cy_send, cy_recv, c_local,
    s1_send, s1_recv, s2_send, s2_recv, h1_send, h1_recv, m_send, m_recv,
    row_send, row_recv, face_send, face_recv, known_sem,
):
    depth, strip, width = nrm.shape
    spd, samples = src.shape[0], src.shape[1]
    box_rows = src.shape[3]
    halves = width // LANES
    whole, split = plan(depth)
    block = min(box_rows, strip)
    per_strip = strip // block
    half_ns = ns // 2
    half_nt = nt // 2
    shot = lax.axis_index("shot")
    tile = lax.axis_index("tile")
    core = lax.rem(shot, 2)
    pair = shot // 2
    other = 1 - core
    mine = lax.rem(tile, half_nt)
    base = tile - mine
    mirror = lax.rem(tile + half_nt, nt)
    twin = {"shot": 2 * pair + other}
    nb = len(split)
    far = range(nb)
    own = range(nb, 2 * nb)
    plane = split + split

    def peer_shot(m):
        return {"shot": 2 * lax.rem(pair + m, half_ns) + core}

    def slab_of(u, to):
        return lax.rem(to + half_nt, nt) if u in far else to

    barrier = pltpu.get_barrier_semaphore()
    for k in range(1, ns):
        pl.semaphore_signal(barrier, inc=1, device_id={"shot": lax.rem(shot + k, ns)})
    column, side = tile // 2, lax.rem(tile, 2)
    columns = nt // 2
    around = (
        (None, {"tile": tile + 1 - 2 * side}),
        (column > 0, {"tile": lax.rem(tile + nt - 2, nt)}),
        (column < columns - 1, {"tile": lax.rem(tile + 2, nt)}),
    )

    def greet(sem):
        for there, who in around:
            if there is None:
                pl.semaphore_signal(sem, inc=1, device_id=who)
            else:
                @pl.when(there)
                def _(who=who):
                    pl.semaphore_signal(sem, inc=1, device_id=who)

    def await_greetings(sem, more):
        pl.semaphore_wait(sem, more + 1 + jnp.minimum(column, 1) + jnp.minimum(columns - 1 - column, 1))

    def learn(r):
        await_greetings(known_sem.at[r], 0)
        if r + 1 < known_sem.shape[0]:
            greet(known_sem.at[r + 1])

    greet(barrier)

    for w, ref in enumerate((src, rcv)):
        for i in range(spd):
            for n in range(samples):
                pltpu.make_async_copy(ref.at[i, n], sbuf.at[:, w, i, n], in_sem).start()
    pltpu.make_async_copy(cor, cbuf.at[tile], c_recv).start()
    pltpu.make_async_copy(cor, cby.at[0, mine], cn_recv).start()
    for w, ref in enumerate((src, rcv)):
        for u, p in enumerate(plane):
            pltpu.make_async_copy(
                ref.at[:, :, slab_of(u, tile) * depth + p], rxh.at[u, 0, mine, w], rxh_recv.at[u, 0]
            ).start()
        for u, p in enumerate(whole):
            pltpu.make_async_copy(ref.at[:, :, tile * depth + p], rxw.at[u, tile, w], rxw_recv.at[u]).start()

    await_greetings(barrier, ns - 1)
    greet(known_sem.at[0])
    pltpu.make_async_copy(sbuf, sbuf, in_sem).wait()

    def remote(src_ref, dst_ref, send_sem, recv_sem, device_id):
        pltpu.make_async_remote_copy(
            src_ref=src_ref, dst_ref=dst_ref, send_sem=send_sem, recv_sem=recv_sem, device_id=device_id
        ).start()

    def steps(to):
        return abs(to // 2 - column) + abs(lax.rem(to, 2) - side)

    def near_half(u, when=None, first=1, stop=half_nt):
        for k in range(first, stop):
            to = base + partner(mine, k, half_nt)
            guarded(when, to, lambda k=k, to=to: remote(
                sbuf.at[slab_of(u, to) * depth + plane[u]], rxh.at[u, 0, mine],
                rxh_send.at[u], rxh_recv.at[u, k], {"tile": to},
            ))

    def guarded(when, to, send):
        if when is None:
            send()
        else:
            @pl.when(when(steps(to)))
            def _():
                send()

    def own_half(u):
        for m in range(1, half_ns):
            remote(
                sbuf.at[slab_of(u, tile) * depth + plane[u]], rxh.at[u, m, mine],
                ry_send.at[u], ry_recv.at[u], peer_shot(m),
            )

    def relay(u, first=1, stop=half_nt):
        for k in range(first, stop):
            slot = partner_back(mine, k, half_nt)
            got = rxh.at[u, 0, slot]
            pltpu.make_async_copy(got, got, rxh_recv.at[u, k]).wait()
            for m in range(1, half_ns):
                remote(got, rxh.at[u, m, slot], ry_send.at[u], ry_recv.at[u], peer_shot(m))

    def near_whole(u, when=None):
        for k in range(1, half_nt):
            to = base + partner(mine, k, half_nt)
            guarded(when, to, lambda to=to: remote(
                sbuf.at[to * depth + whole[u]], rxw.at[u, tile], rxw_send.at[u], rxw_recv.at[u], {"tile": to}
            ))

    def far_whole(u, when=None):
        for k in range(half_nt):
            to = (half_nt - base) + partner(mine, k, half_nt)
            guarded(when, to, lambda to=to: remote(
                sbuf.at[to * depth + whole[u]], rxw.at[u, tile], rxw_send.at[u], rxw_recv.at[u], {"tile": to}
            ))

    def corners(when):
        for k in range(1, half_nt):
            to = base + partner(mine, k, half_nt)
            guarded(when, to, lambda to=to: remote(cor, cby.at[0, mine], cn_send, cn_recv, {"tile": to}))
        for k in range(1, nt):
            to = partner(tile, k, nt)
            guarded(when, to, lambda to=to: remote(cor, cbuf.at[tile], c_send, c_recv, {"tile": to}))

    early = own

    def early_half(when):
        for u in early:
            near_half(u, when, 1, 2)

    for level in (1, 2, 3):
        if level == 1:
            when = lambda d: d == 1
        elif level == 2:
            learn(0)
            when = lambda d: d == 2
        else:
            for r in range(1, known_sem.shape[0]):
                learn(r)
            when = lambda d: d > 2
        corners(when)
        near_half(far[0], when)
        far_whole(0, when)
        if level == 1:
            for u in range(2 * nb):
                own_half(u)
        early_half(when)
        near_whole(0, when)
        if level in (1,):
            far_whole(1, when)
    for u in far[1:]:
        near_half(u, None, 1)
    far_whole(1, lambda d: d > 1)
    near_whole(1)
    for u in own:
        near_half(u, None, 2)

    edges = (
        (shot < ns - 1, shot > 0, {"shot": lax.rem(shot + 1, ns)}),
        (shot > 0, shot < ns - 1, {"shot": lax.rem(shot + ns - 1, ns)}),
    )
    faces = (
        (tile < nt - 1, tile > 0, {"tile": lax.rem(tile + 1, nt)}, depth - 1),
        (tile > 0, tile < nt - 1, {"tile": lax.rem(tile + nt - 1, nt)}, 0),
    )
    for d in range(2):
        @pl.when(jnp.logical_not(edges[d][1]))
        def _(d=d):
            hx[d] = jnp.zeros((depth, 1, width), jnp.float32)

    def edge_copy(d, p):
        return pltpu.make_async_remote_copy(
            src_ref=rows.at[d, p], dst_ref=hx.at[d, p],
            send_sem=row_send.at[d, p], recv_sem=row_recv.at[d, p], device_id=edges[d][2],
        )

    def face_copy(d):
        return pltpu.make_async_remote_copy(
            src_ref=nrm.at[faces[d][3]], dst_ref=hz.at[d],
            send_sem=face_send.at[d], recv_sem=face_recv.at[d], device_id=faces[d][2],
        )

    def cross_copies(n):
        pieces = []
        for g, (a, b) in enumerate(((mbuf, mx), (mhal, mhx))):
            pieces.append(pltpu.make_async_remote_copy(
                src_ref=a.at[n], dst_ref=b.at[n],
                send_sem=m_send.at[n, g], recv_sem=m_recv.at[n, g], device_id={"tile": mirror},
            ))
        return pieces

    zero = jnp.zeros((block, LANES), jnp.float32)

    def clear(s, carry):
        for q in range(2):
            for h in range(halves):
                boxes[s, q, h, pl.ds(0, block), :] = zero
                boxes[s, q, h, pl.ds(block + box_rows, block), :] = zero
        return carry

    lax.fori_loop(0, boxes.shape[0], clear, 0)

    lane = lax.broadcasted_iota(jnp.int32, (box_rows, LANES), 1)

    def expand_one(s, col, wave_of, back_of):
        turn = lax.rem(col, LANES)
        image = jnp.zeros((box_rows, LANES), jnp.float32)
        light = image
        for n in range(samples):
            wave = wave_of(n).astype(jnp.float32)
            back = back_of(n).astype(jnp.float32)
            image = wave * back if n == 0 else image + wave * back
            light = wave * wave if n == 0 else light + wave * wave
        image = pltpu.roll(image, turn, 1)
        light = pltpu.roll(light, turn, 1)
        for h in range(halves):
            at = lane + (h * LANES - col)
            inside = (at >= 0) & (at < LANES)
            boxes[s, 0, h, pl.ds(block, box_rows), :] = jnp.where(inside, image, 0.0)
            boxes[s, 1, h, pl.ds(block, box_rows), :] = jnp.where(inside, light, 0.0)

    def expand_whole(u):
        def peer(t, carry):
            for i in range(spd):
                expand_one(
                    t * spd + i, csm[t, i, 1],
                    lambda n: rxw[u, t, 0, i, n], lambda n: rxw[u, t, 1, i, n],
                )
            return carry

        lax.fori_loop(0, nt, peer, 0)

    def expand_half(u, first, stop):
        for m in range(first, stop):
            def peer(t, carry):
                for i in range(spd):
                    expand_one(
                        (m * half_nt + t) * spd + i, csy[m, t, i, 1],
                        lambda n: rxh[u, m, t, 0, i, n], lambda n: rxh[u, m, t, 1, i, n],
                    )
                return carry

            lax.fori_loop(0, half_nt, peer, 0)

    whole_rows = [(s, lambda s=s: csm[s // spd, s % spd, 0]) for s in range(nt * spd)]
    half_rows = [
        ((m * half_nt + t) * spd + i, lambda m=m, t=t, i=i: csy[m, t, i, 0])
        for m in range(half_ns) for t in range(half_nt) for i in range(spd)
    ]

    def stack(corner_rows, first, count):
        total = [[None] * halves for _ in range(2)]
        for s, corner in corner_rows:
            start = jnp.clip(first + block - corner(), 0, box_rows + block)
            for q in range(2):
                for h in range(halves):
                    piece = boxes[s, q, h, pl.ds(start, count), :]
                    total[q][h] = piece if total[q][h] is None else total[q][h] + piece
        return total

    def place_whole(u, parity, k, count):
        def one(n, carry):
            j = 2 * lax.rem(pair + k + n // per_strip, half_ns) + parity
            at = lax.rem(n, per_strip) * block
            total = stack(whole_rows, j * strip + at, block)
            for q in range(2):
                for h in range(halves):
                    acc[u, j, q, pl.ds(at, block), pl.ds(h * LANES, LANES)] = total[q][h]
            return carry

        lax.fori_loop(0, count * per_strip, one, 0)

    def place_half(u, parity):
        top = (2 * pair + parity) * strip

        def one(n, carry):
            at = n * block
            total = stack(half_rows, top + at, block)
            for q in range(2):
                for h in range(halves):
                    hacc[u, parity, q, pl.ds(at, block), pl.ds(h * LANES, LANES)] = total[q][h]
            return carry

        lax.fori_loop(0, per_strip, one, 0)
        for d, first in enumerate((top - 1, top + strip)):
            total = stack(half_rows, first, 1)
            for q in range(2):
                for h in range(halves):
                    hal[u, parity, pl.ds(2 * q + d, 1), pl.ds(h * LANES, LANES)] = total[q][h]

    def receive_whole(u):
        pltpu.make_async_copy(rxw.at[u], rxw.at[u], rxw_recv.at[u]).wait()
        expand_whole(u)

    def spread_whole(u):
        for k in range(1, half_ns + 1):
            i = lax.rem(pair + k, half_ns)
            place_whole(u, other, k, 1)
            remote(acc.at[u, 2 * i + other], r1.at[u, i], s1_send.at[u, k - 1], s1_recv.at[u, k - 1], twin)
        place_whole(u, core, 1, half_ns)

    def wait_first(u, k):
        got = r1.at[u, lax.rem(pair + k, half_ns)]
        pltpu.make_async_copy(got, got, s1_recv.at[u, k - 1]).wait()

    def gather_whole(u):
        receive_whole(u)
        spread_whole(u)

    def gather_half(u):
        got = rxh.at[u, 0, mine]
        pltpu.make_async_copy(got, got, rxh_recv.at[u, 0]).wait()
        expand_half(u, 0, 1)
        got = rxh.at[u, pl.ds(1, half_ns - 1)]
        pltpu.make_async_copy(got, got, ry_recv.at[u]).wait()
        expand_half(u, 1, half_ns)
        place_half(u, other)
        remote(hacc.at[u, other], hr1.at[u], h1_send.at[u, 0], h1_recv.at[u, 0], twin)
        remote(hal.at[u, other], hal1.at[u], h1_send.at[u, 1], h1_recv.at[u, 1], twin)
        place_half(u, core)

    def wait_twin(u):
        pltpu.make_async_copy(hr1.at[u], hr1.at[u], h1_recv.at[u, 0]).wait()
        pltpu.make_async_copy(hal1.at[u], hal1.at[u], h1_recv.at[u, 1]).wait()

    def stage2(u):
        for k in range(1, half_ns):
            wait_first(u, k)
            to = lax.rem(pair + k, half_ns)
            j = 2 * to + core
            acc[u, j] = acc[u, j] + r1[u, to]
            remote(acc.at[u, j], r2.at[u, k - 1], s2_send.at[u], s2_recv.at[u], {"shot": j})

    def cross(n):
        u = far[n]
        wait_twin(u)
        mhal[n] = hal[u, core] + hal1[u]
        mbuf[n] = hacc[u, core] + hr1[u]
        for copy in reversed(cross_copies(n)):
            copy.start()

    def finish_whole(u):
        p = whole[u]
        wait_first(u, half_ns)
        pltpu.make_async_copy(r2.at[u], r2.at[u], s2_recv.at[u]).wait()
        image = acc[u, shot, 0] + r1[u, pair, 0]
        light = acc[u, shot, 1] + r1[u, pair, 1]
        for k in range(half_ns - 1):
            image = image + r2[u, k, 0]
            light = light + r2[u, k, 1]
        normal = image / (damping + light)
        nrm[p] = normal
        rows[0, p] = normal[strip - 1 :, :]
        rows[1, p] = normal[:1, :]
        for d in range(2):
            @pl.when(edges[d][0])
            def _(d=d):
                edge_copy(d, p).start()

            if p == faces[d][3]:
                @pl.when(faces[d][0])
                def _(d=d):
                    face_copy(d).start()

    def finish_half(n):
        p, u = split[n], own[n]
        wait_twin(u)
        for copy in cross_copies(n):
            copy.wait_recv()
        image = (hacc[u, core, 0] + hr1[u, 0]) + mx[n, 0]
        light = (hacc[u, core, 1] + hr1[u, 1]) + mx[n, 1]
        nrm[p] = image / (damping + light)
        rim = hal[u, core] + hal1[u] + mhx[n]
        rim = rim[0:2, :] / (damping + rim[2:4, :])
        hx[0, p] = rim[0:1, :]
        hx[1, p] = rim[1:2, :]

    row = lax.broadcasted_iota(jnp.int32, (strip, width), 0)
    lanes = lax.broadcasted_iota(jnp.int32, (strip, width), 1)

    def lateral(p):
        center = nrm[p]
        above = 0.0 if p in whole else hx[0, p]
        below = 0.0 if p in whole else hx[1, p]
        before = jnp.where(row == 0, above, pltpu.roll(center, 1, 0))
        after = jnp.where(row == strip - 1, below, pltpu.roll(center, strip - 1, 0))
        left = jnp.where(lanes == 0, 0.0, pltpu.roll(center, 1, 1))
        right = jnp.where(lanes == width - 1, 0.0, pltpu.roll(center, width - 1, 1))
        return before + after + left + right - 6.0 * center

    def near_planes(p):
        return [q for q in (p - 1, p + 1) if 0 <= q < depth]

    def base_plane(p, known):
        value = lateral(p)
        for q in near_planes(p):
            if q in known:
                value = value + nrm[q]
        out[p] = value

    def add_outside():
        for p in whole:
            for d in range(2):
                @pl.when(edges[d][1])
                def _(d=d):
                    edge_copy(d, p).wait_recv()
            out[p, pl.ds(0, 1), :] = out[p, pl.ds(0, 1), :] + hx[0, p]
            out[p, pl.ds(strip - 1, 1), :] = out[p, pl.ds(strip - 1, 1), :] + hx[1, p]
        for d, p in ((0, 0), (1, depth - 1)):
            @pl.when(faces[d][1])
            def _(d=d, p=p):
                face_copy(d).wait_recv()
                out[p] = out[p] + hz[d]

    last = split[-1]
    middle = split[:-1]

    pltpu.make_async_copy(cby.at[0], cby.at[0], cn_recv).wait()
    for m in range(1, half_ns):
        remote(cby.at[0], cby.at[m], cy_send, cy_recv, peer_shot(m))
    relay(far[0])
    peers = cby.at[pl.ds(1, half_ns - 1)]
    pltpu.make_async_copy(peers, peers, cy_recv).wait()
    half_corners = pltpu.make_async_copy(cby, csy, c_local.at[0])
    half_corners.start()
    for u in early:
        relay(u, 1, 2)
    half_corners.wait()

    gather_half(far[0])
    pltpu.make_async_copy(cbuf, cbuf, c_recv).wait()
    all_corners = pltpu.make_async_copy(cbuf, csm, c_local.at[1])
    all_corners.start()
    for u in far[1:]:
        relay(u, 1)
    all_corners.wait()
    gather_whole(0)
    cross(0)
    stage2(0)
    for n in range(1, nb):
        gather_half(far[n])
    receive_whole(1)
    for n in range(1, nb):
        cross(n)
    spread_whole(1)
    relay(own[0], 2)
    stage2(1)
    for u in own[1:]:
        relay(u, 2)
    finish_whole(0)
    for u in own[:-1]:
        gather_half(u)
    finish_whole(1)
    gather_half(own[nb - 1])
    for n in range(nb - 1):
        finish_half(n)
    known = whole + middle
    for p in known:
        base_plane(p, known)
    finish_half(nb - 1)
    for p in near_planes(last):
        out[p] = out[p] + nrm[last]
    base_plane(last, known)
    add_outside()

    for d in range(2):
        @pl.when(edges[d][0])
        def _(d=d):
            for p in whole:
                edge_copy(d, p).wait_send()

        @pl.when(faces[d][0])
        def _(d=d):
            face_copy(d).wait_send()

    def drain(ref, sem):
        pltpu.make_async_copy(ref, ref, sem).wait()

    drain(cbuf.at[pl.ds(0, nt - 1)], c_send)
    drain(cby.at[0, pl.ds(0, half_nt - 1)], cn_send)
    drain(cby.at[pl.ds(1, half_ns - 1)], cy_send)
    for u in range(len(whole)):
        drain(rxw.at[u, pl.ds(0, nt - 1)], rxw_send.at[u])
        for k in range(half_ns):
            drain(r1.at[u, k], s1_send.at[u, k])
        drain(r2.at[u], s2_send.at[u])
    for u in range(2 * nb):
        drain(rxh.at[u, 0, pl.ds(0, half_nt - 1)], rxh_send.at[u])
        drain(rxh.at[u, pl.ds(1, half_ns - 1)], ry_send.at[u])
        drain(hr1.at[u], h1_send.at[u, 0])
        drain(hal1.at[u], h1_send.at[u, 1])
    for n in range(nb):
        for copy in cross_copies(n):
            copy.wait_send()


def solution(mesh):
    ns, nt = mesh.shape["shot"], mesh.shape["tile"]

    def step(source, receiver, corners):
        spd, samples, full_depth, box_rows, box_cols = source.shape
        depth = full_depth // nt
        strip = X // ns
        block = min(box_rows, strip)
        half_ns = ns // 2
        half_nt = nt // 2
        whole, split = plan(depth)
        nw, nb = len(whole), len(split)
        vmem = pltpu.VMEM
        dma = pltpu.SemaphoreType.DMA
        f32 = jnp.float32
        bf16 = jnp.bfloat16
        waves = (2, spd, samples, box_rows, box_cols)
        return pl.pallas_call(
            functools.partial(kernel, ns, nt),
            out_shape=jax.ShapeDtypeStruct((depth, strip, Y), f32),
            in_specs=[pl.BlockSpec(memory_space=pl.ANY)] * 3,
            out_specs=pl.BlockSpec(memory_space=pltpu.VMEM),
            scratch_shapes=[
                vmem((full_depth, *waves), bf16),
                vmem((nw, nt, *waves), bf16),
                vmem((2 * nb, half_ns, half_nt, *waves), bf16),
                vmem((nt, spd, 2), jnp.int32),
                pltpu.SMEM((nt, spd, 2), jnp.int32),
                vmem((half_ns, half_nt, spd, 2), jnp.int32),
                pltpu.SMEM((half_ns, half_nt, spd, 2), jnp.int32),
                vmem((max(nt, half_ns * half_nt) * spd, 2, Y // LANES, box_rows + 2 * block, LANES), f32),
                vmem((nw, ns, 2, strip, Y), f32),
                vmem((nw, half_ns, 2, strip, Y), f32),
                vmem((nw, half_ns - 1, 2, strip, Y), f32),
                vmem((2 * nb, 2, 2, strip, Y), f32),
                vmem((2 * nb, 2, strip, Y), f32),
                vmem((2 * nb, 2, 4, Y), f32),
                vmem((2 * nb, 4, Y), f32),
                vmem((nb, 2, strip, Y), f32),
                vmem((nb, 2, strip, Y), f32),
                vmem((nb, 4, Y), f32),
                vmem((nb, 4, Y), f32),
                vmem((depth, strip, Y), f32),
                vmem((2, depth, 1, Y), f32),
                vmem((2, strip, Y), f32),
                vmem((2, depth, 1, Y), f32),
                dma,
                dma((nw,)),
                dma((nw,)),
                dma((2 * nb,)),
                dma((2 * nb, half_nt)),
                dma((2 * nb,)),
                dma((2 * nb,)),
                dma,
                dma,
                dma,
                dma,
                dma,
                dma,
                dma((2,)),
                dma((nw, half_ns)),
                dma((nw, half_ns)),
                dma((nw,)),
                dma((nw,)),
                dma((2 * nb, 2)),
                dma((2 * nb, 2)),
                dma((nb, 2)),
                dma((nb, 2)),
                dma((2, depth)),
                dma((2, depth)),
                dma((2,)),
                dma((2,)),
                pltpu.SemaphoreType.REGULAR((nt // 2 - 1,)),
            ],
            compiler_params=pltpu.CompilerParams(
                collective_id=0, has_side_effects=True, vmem_limit_bytes=54700 * 1024
            ),
        )(source, receiver, corners)

    return jax.shard_map(
        step,
        mesh=mesh,
        in_specs=(
            P(("shot", "tile"), None, None, None, None),
            P(("shot", "tile"), None, None, None, None),
            P(("shot", "tile"), None),
        ),
        out_specs=P("tile", "shot", None),
        check_vma=False,
    )
```

```python
import functools

import jax
import jax.numpy as jnp
from jax import lax
from jax.experimental import pallas as pl
from jax.experimental.pallas import tpu as pltpu
from jax.sharding import PartitionSpec as P

X = 256
Y = 256
LANES = 128

damping = 1.0


def partner(index, k, count):
    if count & (count - 1):
        return lax.rem(index + k, count)
    bit = 1
    result = index
    while bit < count:
        if k & bit:
            result = result + bit * (1 - 2 * lax.rem(index // bit, 2))
        bit *= 2
    return result


def partner_back(index, k, count):
    if count & (count - 1):
        return lax.rem(index + count - k, count)
    return partner(index, k, count)


def plan(depth):
    if depth < 3:
        return list(range(depth)), []
    return [0, depth - 1], list(range(1, depth - 1))


def kernel(
    ns, nt, src, rcv, cor, out, sbuf, rxw, rxh, cbuf, csm, cby, csy, boxes,
    acc, r1, r2, hacc, hr1, hal, hal1, mbuf, mx, mhal, mhx, nrm, hx, hz, rows,
    in_sem, rxw_send, rxw_recv, rxh_send, rxh_recv, ry_send, ry_recv,
    c_send, c_recv, cn_send, cn_recv, cy_send, cy_recv, c_local,
    s1_send, s1_recv, s2_send, s2_recv, h1_send, h1_recv, m_send, m_recv,
    row_send, row_recv, face_send, face_recv, known_sem,
):
    depth, strip, width = nrm.shape
    spd, samples = src.shape[0], src.shape[1]
    box_rows = src.shape[3]
    halves = width // LANES
    whole, split = plan(depth)
    block = min(box_rows, strip)
    per_strip = strip // block
    half_ns = ns // 2
    half_nt = nt // 2
    shot = lax.axis_index("shot")
    tile = lax.axis_index("tile")
    core = lax.rem(shot, 2)
    pair = shot // 2
    other = 1 - core
    mine = lax.rem(tile, half_nt)
    base = tile - mine
    mirror = lax.rem(tile + half_nt, nt)
    twin = {"shot": 2 * pair + other}
    nb = len(split)
    far = range(nb)
    own = range(nb, 2 * nb)
    plane = split + split

    def peer_shot(m):
        return {"shot": 2 * lax.rem(pair + m, half_ns) + core}

    def slab_of(u, to):
        return lax.rem(to + half_nt, nt) if u in far else to

    barrier = pltpu.get_barrier_semaphore()
    for k in range(1, ns):
        pl.semaphore_signal(barrier, inc=1, device_id={"shot": lax.rem(shot + k, ns)})
    column, side = tile // 2, lax.rem(tile, 2)
    columns = nt // 2
    around = (
        (None, {"tile": tile + 1 - 2 * side}),
        (column > 0, {"tile": lax.rem(tile + nt - 2, nt)}),
        (column < columns - 1, {"tile": lax.rem(tile + 2, nt)}),
    )

    def greet(sem):
        for there, who in around:
            if there is None:
                pl.semaphore_signal(sem, inc=1, device_id=who)
            else:
                @pl.when(there)
                def _(who=who):
                    pl.semaphore_signal(sem, inc=1, device_id=who)

    def await_greetings(sem, more):
        pl.semaphore_wait(sem, more + 1 + jnp.minimum(column, 1) + jnp.minimum(columns - 1 - column, 1))

    def learn(r):
        await_greetings(known_sem.at[r], 0)
        if r + 1 < known_sem.shape[0]:
            greet(known_sem.at[r + 1])

    greet(barrier)

    for w, ref in enumerate((src, rcv)):
        for i in range(spd):
            for n in range(samples):
                pltpu.make_async_copy(ref.at[i, n], sbuf.at[:, w, i, n], in_sem).start()
    pltpu.make_async_copy(cor, cbuf.at[tile], c_recv).start()
    pltpu.make_async_copy(cor, cby.at[0, mine], cn_recv).start()
    for w, ref in enumerate((src, rcv)):
        for u, p in enumerate(plane):
            pltpu.make_async_copy(
                ref.at[:, :, slab_of(u, tile) * depth + p], rxh.at[u, 0, mine, w], rxh_recv.at[u, 0]
            ).start()
        for u, p in enumerate(whole):
            pltpu.make_async_copy(ref.at[:, :, tile * depth + p], rxw.at[u, tile, w], rxw_recv.at[u]).start()

    await_greetings(barrier, ns - 1)
    greet(known_sem.at[0])
    pltpu.make_async_copy(sbuf, sbuf, in_sem).wait()

    def remote(src_ref, dst_ref, send_sem, recv_sem, device_id):
        pltpu.make_async_remote_copy(
            src_ref=src_ref, dst_ref=dst_ref, send_sem=send_sem, recv_sem=recv_sem, device_id=device_id
        ).start()

    def steps(to):
        return abs(to // 2 - column) + abs(lax.rem(to, 2) - side)

    def near_half(u, when=None, first=1, stop=half_nt):
        for k in range(first, stop):
            to = base + partner(mine, k, half_nt)
            guarded(when, to, lambda k=k, to=to: remote(
                sbuf.at[slab_of(u, to) * depth + plane[u]], rxh.at[u, 0, mine],
                rxh_send.at[u], rxh_recv.at[u, k], {"tile": to},
            ))

    def guarded(when, to, send):
        if when is None:
            send()
        else:
            @pl.when(when(steps(to)))
            def _():
                send()

    def own_half(u):
        for m in range(1, half_ns):
            remote(
                sbuf.at[slab_of(u, tile) * depth + plane[u]], rxh.at[u, m, mine],
                ry_send.at[u], ry_recv.at[u], peer_shot(m),
            )

    def relay(u, first=1, stop=half_nt):
        for k in range(first, stop):
            slot = partner_back(mine, k, half_nt)
            got = rxh.at[u, 0, slot]
            pltpu.make_async_copy(got, got, rxh_recv.at[u, k]).wait()
            for m in range(1, half_ns):
                remote(got, rxh.at[u, m, slot], ry_send.at[u], ry_recv.at[u], peer_shot(m))

    def near_whole(u, when=None):
        for k in range(1, half_nt):
            to = base + partner(mine, k, half_nt)
            guarded(when, to, lambda to=to: remote(
                sbuf.at[to * depth + whole[u]], rxw.at[u, tile], rxw_send.at[u], rxw_recv.at[u], {"tile": to}
            ))

    def far_whole(u, when=None):
        for k in range(half_nt):
            to = (half_nt - base) + partner(mine, k, half_nt)
            guarded(when, to, lambda to=to: remote(
                sbuf.at[to * depth + whole[u]], rxw.at[u, tile], rxw_send.at[u], rxw_recv.at[u], {"tile": to}
            ))

    def corners(when):
        for k in range(1, half_nt):
            to = base + partner(mine, k, half_nt)
            guarded(when, to, lambda to=to: remote(cor, cby.at[0, mine], cn_send, cn_recv, {"tile": to}))
        for k in range(1, nt):
            to = partner(tile, k, nt)
            guarded(when, to, lambda to=to: remote(cor, cbuf.at[tile], c_send, c_recv, {"tile": to}))

    early = own

    def early_half(when):
        for u in early:
            near_half(u, when, 1, 2)

    for level in (1, 2, 3):
        if level == 1:
            when = lambda d: d == 1
        elif level == 2:
            learn(0)
            when = lambda d: d == 2
        else:
            for r in range(1, known_sem.shape[0]):
                learn(r)
            when = lambda d: d > 2
        corners(when)
        near_half(far[0], when)
        far_whole(0, when)
        if level == 1:
            for u in range(2 * nb):
                own_half(u)
        early_half(when)
        for u in far[1:]:
            near_half(u, when)
        if level in (1,):
            far_whole(1, when)
    near_whole(0)
    far_whole(1, lambda d: d > 1)
    near_whole(1)
    for u in own:
        near_half(u, None, 2)

    edges = (
        (shot < ns - 1, shot > 0, {"shot": lax.rem(shot + 1, ns)}),
        (shot > 0, shot < ns - 1, {"shot": lax.rem(shot + ns - 1, ns)}),
    )
    faces = (
        (tile < nt - 1, tile > 0, {"tile": lax.rem(tile + 1, nt)}, depth - 1),
        (tile > 0, tile < nt - 1, {"tile": lax.rem(tile + nt - 1, nt)}, 0),
    )
    for d in range(2):
        @pl.when(jnp.logical_not(edges[d][1]))
        def _(d=d):
            hx[d] = jnp.zeros((depth, 1, width), jnp.float32)

        @pl.when(jnp.logical_not(faces[d][1]))
        def _(d=d):
            hz[d] = jnp.zeros((strip, width), jnp.float32)

    def edge_copy(d, p):
        return pltpu.make_async_remote_copy(
            src_ref=rows.at[d, p], dst_ref=hx.at[d, p],
            send_sem=row_send.at[d, p], recv_sem=row_recv.at[d, p], device_id=edges[d][2],
        )

    def face_copy(d):
        return pltpu.make_async_remote_copy(
            src_ref=nrm.at[faces[d][3]], dst_ref=hz.at[d],
            send_sem=face_send.at[d], recv_sem=face_recv.at[d], device_id=faces[d][2],
        )

    def cross_copies(n):
        pieces = []
        for g, (a, b) in enumerate(((mbuf, mx), (mhal, mhx))):
            pieces.append(pltpu.make_async_remote_copy(
                src_ref=a.at[n], dst_ref=b.at[n],
                send_sem=m_send.at[n, g], recv_sem=m_recv.at[n, g], device_id={"tile": mirror},
            ))
        return pieces

    zero = jnp.zeros((block, LANES), jnp.float32)

    def clear(s, carry):
        for q in range(2):
            for h in range(halves):
                boxes[s, q, h, pl.ds(0, block), :] = zero
                boxes[s, q, h, pl.ds(block + box_rows, block), :] = zero
        return carry

    lax.fori_loop(0, boxes.shape[0], clear, 0)

    lane = lax.broadcasted_iota(jnp.int32, (box_rows, LANES), 1)

    def expand_one(s, col, wave_of, back_of):
        turn = lax.rem(col, LANES)
        image = jnp.zeros((box_rows, LANES), jnp.float32)
        light = image
        for n in range(samples):
            wave = wave_of(n).astype(jnp.float32)
            back = back_of(n).astype(jnp.float32)
            image = wave * back if n == 0 else image + wave * back
            light = wave * wave if n == 0 else light + wave * wave
        image = pltpu.roll(image, turn, 1)
        light = pltpu.roll(light, turn, 1)
        for h in range(halves):
            at = lane + (h * LANES - col)
            inside = (at >= 0) & (at < LANES)
            boxes[s, 0, h, pl.ds(block, box_rows), :] = jnp.where(inside, image, 0.0)
            boxes[s, 1, h, pl.ds(block, box_rows), :] = jnp.where(inside, light, 0.0)

    def expand_whole(u):
        def peer(t, carry):
            for i in range(spd):
                expand_one(
                    t * spd + i, csm[t, i, 1],
                    lambda n: rxw[u, t, 0, i, n], lambda n: rxw[u, t, 1, i, n],
                )
            return carry

        lax.fori_loop(0, nt, peer, 0)

    def expand_half(u, first, stop):
        for m in range(first, stop):
            def peer(t, carry):
                for i in range(spd):
                    expand_one(
                        (m * half_nt + t) * spd + i, csy[m, t, i, 1],
                        lambda n: rxh[u, m, t, 0, i, n], lambda n: rxh[u, m, t, 1, i, n],
                    )
                return carry

            lax.fori_loop(0, half_nt, peer, 0)

    whole_rows = [(s, lambda s=s: csm[s // spd, s % spd, 0]) for s in range(nt * spd)]
    half_rows = [
        ((m * half_nt + t) * spd + i, lambda m=m, t=t, i=i: csy[m, t, i, 0])
        for m in range(half_ns) for t in range(half_nt) for i in range(spd)
    ]

    def stack(corner_rows, first, count):
        total = [[None] * halves for _ in range(2)]
        for s, corner in corner_rows:
            start = jnp.clip(first + block - corner(), 0, box_rows + block)
            for q in range(2):
                for h in range(halves):
                    piece = boxes[s, q, h, pl.ds(start, count), :]
                    total[q][h] = piece if total[q][h] is None else total[q][h] + piece
        return total

    def place_whole(u, parity):
        def one(n, carry):
            j = 2 * (n // per_strip) + parity
            at = lax.rem(n, per_strip) * block
            total = stack(whole_rows, j * strip + at, block)
            for q in range(2):
                for h in range(halves):
                    acc[u, j, q, pl.ds(at, block), pl.ds(h * LANES, LANES)] = total[q][h]
            return carry

        lax.fori_loop(0, half_ns * per_strip, one, 0)

    def place_half(u, parity):
        top = (2 * pair + parity) * strip

        def one(n, carry):
            at = n * block
            total = stack(half_rows, top + at, block)
            for q in range(2):
                for h in range(halves):
                    hacc[u, parity, q, pl.ds(at, block), pl.ds(h * LANES, LANES)] = total[q][h]
            return carry

        lax.fori_loop(0, per_strip, one, 0)
        for d, first in enumerate((top - 1, top + strip)):
            total = stack(half_rows, first, 1)
            for q in range(2):
                for h in range(halves):
                    hal[u, parity, pl.ds(2 * q + d, 1), pl.ds(h * LANES, LANES)] = total[q][h]

    def receive_whole(u):
        pltpu.make_async_copy(rxw.at[u], rxw.at[u], rxw_recv.at[u]).wait()
        expand_whole(u)

    def spread_whole(u):
        place_whole(u, other)
        for i in range(half_ns):
            remote(acc.at[u, 2 * i + other], r1.at[u, i], s1_send.at[u], s1_recv.at[u], twin)
        place_whole(u, core)

    def gather_whole(u):
        receive_whole(u)
        spread_whole(u)

    def gather_half(u):
        got = rxh.at[u, 0, mine]
        pltpu.make_async_copy(got, got, rxh_recv.at[u, 0]).wait()
        expand_half(u, 0, 1)
        got = rxh.at[u, pl.ds(1, half_ns - 1)]
        pltpu.make_async_copy(got, got, ry_recv.at[u]).wait()
        expand_half(u, 1, half_ns)
        place_half(u, other)
        remote(hacc.at[u, other], hr1.at[u], h1_send.at[u, 0], h1_recv.at[u, 0], twin)
        remote(hal.at[u, other], hal1.at[u], h1_send.at[u, 1], h1_recv.at[u, 1], twin)
        place_half(u, core)

    def wait_twin(u):
        pltpu.make_async_copy(hr1.at[u], hr1.at[u], h1_recv.at[u, 0]).wait()
        pltpu.make_async_copy(hal1.at[u], hal1.at[u], h1_recv.at[u, 1]).wait()

    def stage2(u):
        pltpu.make_async_copy(r1.at[u], r1.at[u], s1_recv.at[u]).wait()
        for k in range(1, half_ns):
            to = lax.rem(pair + k, half_ns)
            j = 2 * to + core
            acc[u, j] = acc[u, j] + r1[u, to]
            remote(acc.at[u, j], r2.at[u, k - 1], s2_send.at[u], s2_recv.at[u], {"shot": j})

    def cross(n):
        u = far[n]
        wait_twin(u)
        mhal[n] = hal[u, core] + hal1[u]
        mbuf[n] = hacc[u, core] + hr1[u]
        for copy in reversed(cross_copies(n)):
            copy.start()

    def finish_whole(u):
        p = whole[u]
        pltpu.make_async_copy(r2.at[u], r2.at[u], s2_recv.at[u]).wait()
        image = acc[u, shot, 0] + r1[u, pair, 0]
        light = acc[u, shot, 1] + r1[u, pair, 1]
        for k in range(half_ns - 1):
            image = image + r2[u, k, 0]
            light = light + r2[u, k, 1]
        normal = image / (damping + light)
        nrm[p] = normal
        rows[0, p] = normal[strip - 1 :, :]
        rows[1, p] = normal[:1, :]
        for d in range(2):
            @pl.when(edges[d][0])
            def _(d=d):
                edge_copy(d, p).start()

            if p == faces[d][3]:
                @pl.when(faces[d][0])
                def _(d=d):
                    face_copy(d).start()

    def finish_half(n):
        p, u = split[n], own[n]
        wait_twin(u)
        for copy in cross_copies(n):
            copy.wait_recv()
        image = (hacc[u, core, 0] + hr1[u, 0]) + mx[n, 0]
        light = (hacc[u, core, 1] + hr1[u, 1]) + mx[n, 1]
        nrm[p] = image / (damping + light)
        rim = hal[u, core] + hal1[u] + mhx[n]
        rim = rim[0:2, :] / (damping + rim[2:4, :])
        hx[0, p] = rim[0:1, :]
        hx[1, p] = rim[1:2, :]

    row = lax.broadcasted_iota(jnp.int32, (strip, width), 0)
    lanes = lax.broadcasted_iota(jnp.int32, (strip, width), 1)

    def lateral(p):
        center = nrm[p]
        before = jnp.where(row == 0, hx[0, p], pltpu.roll(center, 1, 0))
        after = jnp.where(row == strip - 1, hx[1, p], pltpu.roll(center, strip - 1, 0))
        left = jnp.where(lanes == 0, 0.0, pltpu.roll(center, 1, 1))
        right = jnp.where(lanes == width - 1, 0.0, pltpu.roll(center, width - 1, 1))
        return before + after + left + right - 6.0 * center

    def near_planes(p):
        return [q for q in (p - 1, p + 1) if 0 <= q < depth]

    def base_plane(p, known):
        if p in whole:
            for d in range(2):
                @pl.when(edges[d][1])
                def _(d=d):
                    edge_copy(d, p).wait_recv()
        value = lateral(p)
        for q in near_planes(p):
            if q in known:
                value = value + nrm[q]
        for d in range(2):
            if p == (depth - 1 if d else 0):
                @pl.when(faces[d][1])
                def _(d=d):
                    face_copy(d).wait_recv()
                value = value + hz[d]
        out[p] = value

    last = split[-1]
    middle = split[:-1]

    pltpu.make_async_copy(cby.at[0], cby.at[0], cn_recv).wait()
    for m in range(1, half_ns):
        remote(cby.at[0], cby.at[m], cy_send, cy_recv, peer_shot(m))
    relay(far[0])
    peers = cby.at[pl.ds(1, half_ns - 1)]
    pltpu.make_async_copy(peers, peers, cy_recv).wait()
    half_corners = pltpu.make_async_copy(cby, csy, c_local.at[0])
    half_corners.start()
    for u in early:
        relay(u, 1, 2)
    half_corners.wait()

    gather_half(far[0])
    pltpu.make_async_copy(cbuf, cbuf, c_recv).wait()
    all_corners = pltpu.make_async_copy(cbuf, csm, c_local.at[1])
    all_corners.start()
    for u in far[1:]:
        relay(u, 1)
    all_corners.wait()
    gather_whole(0)
    cross(0)
    stage2(0)
    for n in range(1, nb):
        gather_half(far[n])
    receive_whole(1)
    for n in range(1, nb):
        cross(n)
    spread_whole(1)
    relay(own[0], 2)
    stage2(1)
    for u in own[1:]:
        relay(u, 2)
    finish_whole(0)
    for u in own[:-1]:
        gather_half(u)
    finish_whole(1)
    gather_half(own[nb - 1])
    for n in range(nb - 1):
        finish_half(n)
    known = whole + middle
    for p in known:
        base_plane(p, known)
    finish_half(nb - 1)
    for p in near_planes(last):
        out[p] = out[p] + nrm[last]
    base_plane(last, known)

    for d in range(2):
        @pl.when(edges[d][0])
        def _(d=d):
            for p in whole:
                edge_copy(d, p).wait_send()

        @pl.when(faces[d][0])
        def _(d=d):
            face_copy(d).wait_send()

    def drain(ref, sem):
        pltpu.make_async_copy(ref, ref, sem).wait()

    drain(cbuf.at[pl.ds(0, nt - 1)], c_send)
    drain(cby.at[0, pl.ds(0, half_nt - 1)], cn_send)
    drain(cby.at[pl.ds(1, half_ns - 1)], cy_send)
    for u in range(len(whole)):
        drain(rxw.at[u, pl.ds(0, nt - 1)], rxw_send.at[u])
        drain(r1.at[u], s1_send.at[u])
        drain(r2.at[u], s2_send.at[u])
    for u in range(2 * nb):
        drain(rxh.at[u, 0, pl.ds(0, half_nt - 1)], rxh_send.at[u])
        drain(rxh.at[u, pl.ds(1, half_ns - 1)], ry_send.at[u])
        drain(hr1.at[u], h1_send.at[u, 0])
        drain(hal1.at[u], h1_send.at[u, 1])
    for n in range(nb):
        for copy in cross_copies(n):
            copy.wait_send()


def solution(mesh):
    ns, nt = mesh.shape["shot"], mesh.shape["tile"]

    def step(source, receiver, corners):
        spd, samples, full_depth, box_rows, box_cols = source.shape
        depth = full_depth // nt
        strip = X // ns
        block = min(box_rows, strip)
        half_ns = ns // 2
        half_nt = nt // 2
        whole, split = plan(depth)
        nw, nb = len(whole), len(split)
        vmem = pltpu.VMEM
        dma = pltpu.SemaphoreType.DMA
        f32 = jnp.float32
        bf16 = jnp.bfloat16
        waves = (2, spd, samples, box_rows, box_cols)
        return pl.pallas_call(
            functools.partial(kernel, ns, nt),
            out_shape=jax.ShapeDtypeStruct((depth, strip, Y), f32),
            in_specs=[pl.BlockSpec(memory_space=pl.ANY)] * 3,
            out_specs=pl.BlockSpec(memory_space=pltpu.VMEM),
            scratch_shapes=[
                vmem((full_depth, *waves), bf16),
                vmem((nw, nt, *waves), bf16),
                vmem((2 * nb, half_ns, half_nt, *waves), bf16),
                vmem((nt, spd, 2), jnp.int32),
                pltpu.SMEM((nt, spd, 2), jnp.int32),
                vmem((half_ns, half_nt, spd, 2), jnp.int32),
                pltpu.SMEM((half_ns, half_nt, spd, 2), jnp.int32),
                vmem((max(nt, half_ns * half_nt) * spd, 2, Y // LANES, box_rows + 2 * block, LANES), f32),
                vmem((nw, ns, 2, strip, Y), f32),
                vmem((nw, half_ns, 2, strip, Y), f32),
                vmem((nw, half_ns - 1, 2, strip, Y), f32),
                vmem((2 * nb, 2, 2, strip, Y), f32),
                vmem((2 * nb, 2, strip, Y), f32),
                vmem((2 * nb, 2, 4, Y), f32),
                vmem((2 * nb, 4, Y), f32),
                vmem((nb, 2, strip, Y), f32),
                vmem((nb, 2, strip, Y), f32),
                vmem((nb, 4, Y), f32),
                vmem((nb, 4, Y), f32),
                vmem((depth, strip, Y), f32),
                vmem((2, depth, 1, Y), f32),
                vmem((2, strip, Y), f32),
                vmem((2, depth, 1, Y), f32),
                dma,
                dma((nw,)),
                dma((nw,)),
                dma((2 * nb,)),
                dma((2 * nb, half_nt)),
                dma((2 * nb,)),
                dma((2 * nb,)),
                dma,
                dma,
                dma,
                dma,
                dma,
                dma,
                dma((2,)),
                dma((nw,)),
                dma((nw,)),
                dma((nw,)),
                dma((nw,)),
                dma((2 * nb, 2)),
                dma((2 * nb, 2)),
                dma((nb, 2)),
                dma((nb, 2)),
                dma((2, depth)),
                dma((2, depth)),
                dma((2,)),
                dma((2,)),
                pltpu.SemaphoreType.REGULAR((nt // 2 - 1,)),
            ],
            compiler_params=pltpu.CompilerParams(
                collective_id=0, has_side_effects=True, vmem_limit_bytes=54700 * 1024
            ),
        )(source, receiver, corners)

    return jax.shard_map(
        step,
        mesh=mesh,
        in_specs=(
            P(("shot", "tile"), None, None, None, None),
            P(("shot", "tile"), None, None, None, None),
            P(("shot", "tile"), None),
        ),
        out_specs=P("tile", "shot", None),
        check_vma=False,
    )
```
